16 devices in a mesh: dp: 4 (over z, y), sp: 4 (over x, core).
Axes of the slice: x: 2, y: 2, z: 2, core: 2. Of those that a mesh axis runs over, the one named last changes fastest.
Arguments:
- x_rows: bfloat16 [32768, 384], P(('dp', 'sp')), parts along dimension 0
- dy_rows: bfloat16 [32768, 384], P(('dp', 'sp')), parts along dimension 0
- ln_gamma: float32 [384], replicated
- ln_beta: float32 [384], replicated
- w_qkv: bfloat16 [384, 1152], replicated
- w_out: bfloat16 [384, 384], replicated
- temperature: float32 [8], replicated
Outputs:
- output 1: bfloat16 [32768, 384], P(('dp', 'sp')), parts along dimension 0
- output 2: bfloat16 [32768, 384], P(('dp', 'sp')), parts along dimension 0
- output 3: bfloat16 [1536, 1152], P(('dp', 'sp')), parts along dimension 0
- output 4: bfloat16 [1536, 384], P(('dp', 'sp')), parts along dimension 0
- output 5: float32 [1536], P('dp'), parts along dimension 0
- output 6: float32 [1536], P('dp'), parts along dimension 0
- output 7: float32 [32], P('dp'), parts along dimension 0
There are 4 independent parts. The reference program is written for one: setup_inputs(seed, part) draws one part's arguments, and reference() takes and returns one part's arrays. A program takes and returns all parts, laid end to end along the dimension named above; an argument that names none is the same for every part.
All inputs are finite; a program needn't handle non-finite values.
Results may differ from the reference program's by a relative error of at most 0.0117443.
Values are sent between devices in bfloat16 or wider.
A program may use at most 1 GiB of HBM per device.

```python
import jax
import jax.numpy as jnp
from jax import lax

TOKENS = 8192
WIDTH = 384
N_HEADS = 8
SEGMENTS = 8
HEAD_DIM = WIDTH // N_HEADS
LN_EPS = 1e-6


def setup_inputs(seed: int = 0, part: int = 0) -> dict:
    part_keys = jax.random.split(jax.random.fold_in(jax.random.key(seed), part), 4)
    shared_keys = jax.random.split(jax.random.key(seed + 1), 5)
    seg_rows = TOKENS // SEGMENTS
    x_means = jnp.repeat(jax.random.normal(part_keys[0], (SEGMENTS, WIDTH), jnp.float32), seg_rows, axis=0)
    x_rows = jax.random.normal(part_keys[1], (TOKENS, WIDTH), jnp.float32) + 2.0 * x_means
    dy_means = jnp.repeat(jax.random.normal(part_keys[2], (SEGMENTS, WIDTH), jnp.float32), seg_rows, axis=0)
    dy_rows = 0.7 * jax.random.normal(part_keys[3], (TOKENS, WIDTH), jnp.float32) + dy_means
    fan_scale = WIDTH ** -0.5
    ln_gamma = 1.0 + 0.3 * jax.random.normal(shared_keys[0], (WIDTH,), jnp.float32)
    ln_beta = 0.3 * jax.random.normal(shared_keys[1], (WIDTH,), jnp.float32)
    w_qkv = fan_scale * jax.random.normal(shared_keys[2], (WIDTH, 3 * WIDTH), jnp.float32)
    w_out = 1.5 * fan_scale * jax.random.normal(shared_keys[3], (WIDTH, WIDTH), jnp.float32)
    temperature = jax.random.uniform(shared_keys[4], (N_HEADS,), jnp.float32, 3.0, 8.0)
    return {'x_rows': x_rows.astype(jnp.bfloat16), 'dy_rows': dy_rows.astype(jnp.bfloat16), 'ln_gamma': ln_gamma, 'ln_beta': ln_beta, 'w_qkv': w_qkv.astype(jnp.bfloat16), 'w_out': w_out.astype(jnp.bfloat16), 'temperature': temperature}


def xca_forward(x_rows, ln_gamma, ln_beta, w_qkv, w_out, temperature):
    x_f32 = x_rows.astype(jnp.float32)
    row_mean = jnp.mean(x_f32, axis=-1, keepdims=True)
    centered = x_f32 - row_mean
    row_var = jnp.mean(centered * centered, axis=-1, keepdims=True)
    normed = (centered * lax.rsqrt(row_var + LN_EPS) * ln_gamma + ln_beta).astype(jnp.bfloat16)
    qkv_all = jnp.dot(normed, w_qkv, preferred_element_type=jnp.float32).astype(jnp.bfloat16)
    qkv_heads = qkv_all.reshape(TOKENS, 3, N_HEADS, HEAD_DIM).astype(jnp.float32)
    query_h = qkv_heads[:, 0]
    key_h = qkv_heads[:, 1]
    value_h = qkv_heads[:, 2]
    gram = jnp.einsum('nhi,nhj->hij', query_h, key_h)
    q_sq = jnp.sum(query_h * query_h, axis=0)
    k_sq = jnp.sum(key_h * key_h, axis=0)
    scores = temperature[:, None, None] * gram * lax.rsqrt(q_sq)[:, :, None] * lax.rsqrt(k_sq)[:, None, :]
    attn = jax.nn.softmax(scores, axis=-1).astype(jnp.bfloat16)
    attn_out = jnp.einsum('nhj,hij->nhi', value_h, attn.astype(jnp.float32)).astype(jnp.bfloat16)
    proj = jnp.dot(attn_out.reshape(TOKENS, WIDTH), w_out, preferred_element_type=jnp.float32)
    return (x_f32 + proj).astype(jnp.bfloat16)


def reference(x_rows, dy_rows, ln_gamma, ln_beta, w_qkv, w_out, temperature):
    y_rows, backward = jax.vjp(xca_forward, x_rows, ln_gamma, ln_beta, w_qkv, w_out, temperature)
    dx_rows, d_gamma, d_beta, dw_qkv, dw_out, d_temp = backward(dy_rows)
    return (y_rows, dx_rows, dw_qkv, dw_out, d_gamma, d_beta, d_temp)
```

```python
import jax
import jax.numpy as jnp
from jax import lax
from jax.experimental import pallas as pl
from jax.experimental.pallas import tpu as pltpu
from jax.sharding import PartitionSpec as P

LN_EPS = 1e-6
F32 = jnp.float32
BF16 = jnp.bfloat16
N = 2048
D = 384
HD = 48
GW = 192
PW = 256
RB = 96
CH = 256
NCH = N // CH

NN = (((1,), (0,)), ((), ()))
NT = (((1,), (1,)), ((), ()))
TN = (((0,), (0,)), ((), ()))


def mm(a, b, dims):
    return lax.dot_general(a, b, dims, preferred_element_type=F32)


def kernel(x_hbm, dy_hbm, gamma, beta, w_hbm, wo_hbm, temp,
           y_out, dx_out, dw_out, dwo_out, dg_out, db_out, dt_out,
           x, dy, w, wo, wt, u, ut, qkvt, dqkvt, dot_, ot, mean_s, rstd_s, s_acc,
           pk1, pk2, ra, sb, rb, cs, rc, abd, gbd, keep, part, rd1, rd2, ls, rl, es, er,
           in_sem, x_sem, ssem, rsem):
    sp = lax.axis_index("sp")
    core = lax.rem(sp, 2)
    peer = 1 - core
    partner = sp + 1 - 2 * core
    other = lax.rem(sp + 2, 4)
    cross = lax.rem(partner + 2, 4)

    barrier = pltpu.get_barrier_semaphore()
    for dev in (partner, other):
        pl.semaphore_signal(barrier, inc=1, device_id={"sp": dev}, device_id_type=pl.DeviceIdType.MESH)

    w_copy = pltpu.make_async_copy(w_hbm, w, in_sem.at[0])
    wo_copy = pltpu.make_async_copy(wo_hbm, wo, in_sem.at[1])
    dy_copy = pltpu.make_async_copy(dy_hbm, dy, in_sem.at[2])

    def x_copy(i):
        rows = pl.ds(i * CH, CH)
        return pltpu.make_async_copy(x_hbm.at[rows], x.at[rows], x_sem.at[i])

    x_copy(0).start()
    w_copy.start()
    for i in range(1, NCH):
        x_copy(i).start()
    wo_copy.start()
    dy_copy.start()

    def send(slot, src, dst, dev):
        copy = pltpu.make_async_remote_copy(
            src_ref=src, dst_ref=dst, send_sem=ssem.at[slot], recv_sem=rsem.at[slot],
            device_id={"sp": dev}, device_id_type=pl.DeviceIdType.MESH)
        copy.start()
        return copy

    lane = lax.broadcasted_iota(jnp.int32, (HD, PW), 1)
    row = lax.broadcasted_iota(jnp.int32, (HD, PW), 0)
    heads = [(lane >= HD * h) & (lane < HD * h + HD) for h in range(4)]
    eyes = [lane == row + HD * h for h in range(4)]
    valid = lane < GW
    s_acc[...] = jnp.zeros_like(s_acc)
    pk1[...] = jnp.zeros_like(pk1)
    pk2[...] = jnp.zeros_like(pk2)

    def layer_norm(i):
        rows = pl.ds(pl.multiple_of(i * CH, CH), CH)
        xf = x[rows, :].astype(F32)
        mean = jnp.mean(xf, axis=-1, keepdims=True)
        cen = xf - mean
        rstd = lax.rsqrt(jnp.mean(cen * cen, axis=-1, keepdims=True) + LN_EPS)
        mean_s[rows, :] = mean
        rstd_s[rows, :] = rstd
        u[rows, :] = (cen * rstd * gamma[...] + beta[...]).astype(BF16)

    def qk_chunk(i):
        cols = pl.ds(pl.multiple_of(i * CH, CH), CH)
        res = mm(wt[0:2 * D, :], u[cols, :], NT).astype(BF16)
        for s in range(4):
            qkvt[s // 2, s % 2, :, cols] = res[s * GW:(s + 1) * GW]
        sq = jnp.square(res.astype(F32))
        s_acc[...] += sq[:, :128] + sq[:, 128:]

    x_copy(0).wait()
    layer_norm(0)
    w_copy.wait()
    wt[...] = w[...].T

    @pl.loop(0, NCH - 1)
    def _(i):
        rows = pl.ds(pl.multiple_of((i + 1) * CH, CH), CH)
        pltpu.make_async_copy(x_hbm.at[rows], x.at[rows], x_sem.at[i + 1]).wait()
        qk_chunk(i)
        layer_norm(i + 1)

    qk_chunk(NCH - 1)

    def compact(full):
        out = jnp.zeros((HD, GW), F32)
        for h in range(4):
            out = jnp.where(heads[h][:, :GW], full[HD * h:HD * h + HD], out)
        return out

    s_col = jnp.sum(s_acc[...], axis=-1, keepdims=True)
    for g in range(2):
        pk1[g, :, 0:GW] = compact(mm(qkvt[0, g], qkvt[1, g], NT))
        blk = pk1[g]
        for h in range(4):
            r = g * GW + h * HD
            blk = jnp.where(lane == GW + h, s_col[r:r + HD], blk)
            blk = jnp.where(lane == GW + 4 + h, s_col[D + r:D + r + HD], blk)
        pk1[g] = blk

    pl.semaphore_wait(barrier, 2)
    a1 = send(0, pk1.at[peer], ra.at[0], partner)

    CV = 512

    @pl.loop(0, N // CV)
    def _(i):
        cols = pl.ds(pl.multiple_of(i * CV, CV), CV)
        res = mm(wt[2 * D:3 * D, :], u[cols, :], NT).astype(BF16)
        qkvt[2, 0, :, cols] = res[:GW]
        qkvt[2, 1, :, cols] = res[GW:]

    a1.wait_recv()
    sb[0] = pk1[core] + ra[0]
    b1 = send(1, sb.at[0], rb.at[0], other)

    wo_copy.wait()
    dy_copy.wait()

    @pl.loop(0, N // CV)
    def _(i):
        cols = pl.ds(pl.multiple_of(i * CV, CV), CV)
        res = mm(wo[...], dy[cols, :], NT).astype(BF16)
        dot_[0, :, cols] = res[:GW]
        dot_[1, :, cols] = res[GW:]

    for g in range(2):
        pk2[g, :, 0:GW] = compact(mm(dot_[g], qkvt[2, g], NT))
    a2 = send(2, pk2.at[peer], ra.at[1], partner)

    @pl.loop(0, NCH // 2)
    def _(i):
        cols = pl.ds(pl.multiple_of(i * CH, CH), CH)
        ut[:, cols] = u[cols, :].T

    a2.wait_recv()
    sb[1] = pk2[core] + ra[1]
    b2 = send(3, sb.at[1], rb.at[1], other)

    @pl.loop(NCH // 2, NCH)
    def _(i):
        cols = pl.ds(pl.multiple_of(i * CH, CH), CH)
        ut[:, cols] = u[cols, :].T

    def seg_sum(v):
        out = jnp.zeros_like(v)
        for h in range(4):
            out = jnp.where(heads[h], jnp.sum(jnp.where(heads[h], v, 0.0), axis=-1, keepdims=True), out)
        return out

    def expand(dst, g, comp):
        for h in range(4):
            dst[g, HD * h:HD * h + HD, :] = jnp.where(heads[h], comp, 0.0)[:, :GW].astype(BF16)

    b1.wait_recv()
    gs = sb[0] + rb[0]
    rq2 = jnp.zeros((HD, PW), F32)
    rk2 = jnp.zeros((HD, PW), F32)
    tau = jnp.zeros((HD, PW), F32)
    for h in range(4):
        sq_h = jnp.sum(jnp.where(lane == GW + h, gs, 0.0), axis=-1, keepdims=True)
        sk_h = jnp.sum(jnp.where(lane == GW + 4 + h, gs, 0.0), axis=-1, keepdims=True)
        rq2 = jnp.where(heads[h], sq_h, rq2)
        rk2 = jnp.where(eyes[h], sk_h, rk2)
        tau = jnp.where(heads[h], temp[core * 4 + h], tau)
    sk2 = jnp.sum(rk2, axis=0, keepdims=True)
    q_inv = lax.rsqrt(jnp.where(valid, rq2, 1.0))
    k_inv = lax.rsqrt(jnp.where(valid, sk2, 1.0))
    gram = jnp.where(valid, gs, 0.0)
    scores = tau * gram * q_inv * k_inv
    top = jnp.zeros((HD, PW), F32)
    for h in range(4):
        top = jnp.where(heads[h], jnp.max(jnp.where(heads[h], scores, -jnp.inf), axis=-1, keepdims=True), top)
    e = jnp.where(valid, jnp.exp(scores - top), 0.0)
    prob = jnp.where(valid, e / jnp.where(valid, seg_sum(e), 1.0), 0.0)
    cs[0] = prob
    c1 = send(4, cs.at[0], rc.at[0], partner)
    keep[0] = prob
    keep[1] = scores
    keep[2] = gram * q_inv * k_inv
    keep[3] = tau * q_inv * k_inv
    keep[4] = jnp.where(valid, rq2, 1.0)
    keep[5] = jnp.where(valid, jnp.broadcast_to(sk2, (HD, PW)), 1.0)
    expand(abd, core, prob)

    def attend(g):
        ot[g] = mm(abd[g], qkvt[2, g], NN).astype(BF16)

    def d_value(g):
        dqkvt[2, g] = mm(abd[g], dot_[g], TN).astype(BF16)

    attend(core)
    d_value(core)
    c1.wait_recv()
    expand(abd, peer, rc[0])
    attend(peer)

    def all_rows(ref):
        return ref[...].reshape(D, N)

    def weight_send(t):
        return (send(6 + 3 * t, part.at[t, cross], rd1.at[t], partner),
                send(7 + 3 * t, part.at[t, partner], rd2.at[t], partner))

    def link_send(t, first):
        first.wait_recv()
        ls[t] = part[t, other] + rd1[t]
        return send(8 + 3 * t, ls.at[t], rl.at[t], other)

    part[0] = mm(all_rows(ot), dy[...], NN).reshape(4, RB, D)
    d0 = weight_send(0)

    b2.wait_recv()
    da = jnp.where(valid, (sb[1] + rb[1]).astype(BF16).astype(F32), 0.0)
    p = keep[0]
    ds = p * (da - seg_sum(da * p))
    weighted = ds * keep[1]
    dtemp = seg_sum(ds * keep[2])
    dtemp = jnp.sum(dtemp, axis=0, keepdims=True)
    dgram = (ds * keep[3]).astype(BF16).astype(F32)
    dsq = -seg_sum(weighted) / keep[4]
    dsk = -jnp.sum(weighted, axis=0, keepdims=True) / keep[5]
    blk = dgram
    for h in range(4):
        dsk_h = jnp.sum(jnp.where(eyes[h], dsk, 0.0), axis=-1, keepdims=True)
        dsq_h = jnp.sum(jnp.where(eyes[h], dsq, 0.0), axis=-1, keepdims=True)
        dt_h = jnp.sum(jnp.where(lane == HD * h, dtemp, 0.0), axis=-1, keepdims=True)
        blk = jnp.where(lane == GW + h, dsq_h, blk)
        blk = jnp.where(lane == GW + 4 + h, dsk_h, blk)
        blk = jnp.where(lane == GW + 8 + h, dt_h, blk)
    cs[1] = blk
    c2 = send(5, cs.at[1], rc.at[1], partner)

    l0 = link_send(0, d0[0])

    d_value(peer)
    part[1] = mm(all_rows(ut), dqkvt[2].reshape(D, N), NT).reshape(4, RB, D)
    d1 = weight_send(1)

    def d_qk(g, blk):
        expand(gbd, g, jnp.where(valid, blk, 0.0))
        cols = []
        for b in (GW, GW + 4):
            cols.append(jnp.concatenate(
                [jnp.sum(jnp.where(lane == b + h, blk, 0.0), axis=-1, keepdims=True) for h in range(4)], axis=0))
        dqkvt[0, g] = (mm(gbd[g], qkvt[1, g], NN) + qkvt[0, g].astype(F32) * cols[0]).astype(BF16)
        dqkvt[1, g] = (mm(gbd[g], qkvt[0, g], TN) + qkvt[1, g].astype(F32) * cols[1]).astype(BF16)

    d_qk(core, cs[1])
    c2.wait_recv()
    d_qk(peer, rc[1])
    l1 = link_send(1, d1[0])
    part[2] = mm(ut[...], dqkvt[1].reshape(D, N), NT).reshape(4, RB, D)
    d2 = weight_send(2)
    part[3] = mm(ut[...], dqkvt[0].reshape(D, N), NT).reshape(4, RB, D)
    d3 = weight_send(3)
    l2 = link_send(2, d2[0])
    l3 = link_send(3, d3[0])

    lane8 = lax.broadcasted_iota(jnp.int32, (1, 8), 1)
    dt = jnp.zeros((1, 8), F32)
    for g, src in ((core, cs), (peer, rc)):
        head_row = src[1][0:1, :]
        for h in range(4):
            val = jnp.sum(jnp.where(lane[0:1] == GW + 8 + h, head_row, 0.0), axis=-1, keepdims=True)
            dt = jnp.where(lane8 == g * 4 + h, val, dt)
    dt_out[...] = dt

    es[...] = jnp.zeros_like(es)

    @pl.loop(0, NCH)
    def _(i):
        rows = pl.ds(pl.multiple_of(i * CH, CH), CH)
        proj = mm(ot[:, :, rows].reshape(D, CH), wo[...], TN)
        xf = x[rows, :].astype(F32)
        y_out[rows, :] = (xf + proj).astype(BF16)
        dut = mm(w[...], dqkvt[:, :, :, rows].reshape(3 * D, CH), NN).astype(BF16)
        du = dut.T.astype(F32)
        rstd = rstd_s[rows, :]
        xhat = (xf - mean_s[rows, :]) * rstd
        es[0:1, :] += jnp.sum(du * xhat, axis=0, keepdims=True)
        es[1:2, :] += jnp.sum(du, axis=0, keepdims=True)
        dh = du * gamma[...]
        m1 = jnp.mean(dh, axis=-1, keepdims=True)
        m2 = jnp.mean(dh * xhat, axis=-1, keepdims=True)
        dx_out[rows, :] = (dy[rows, :].astype(F32) + rstd * (dh - m1 - xhat * m2)).astype(BF16)

    e1 = send(18, es, er.at[0], partner)
    e1.wait()
    er[1] = es[...] + er[0]
    e2 = send(19, er.at[1], er.at[2], other)

    outs = ((dwo_out, slice(0, D)), (dw_out, slice(2 * D, 3 * D)), (dw_out, slice(D, 2 * D)), (dw_out, slice(0, D)))
    for t, (d, l) in enumerate(((d0, l0), (d1, l1), (d2, l2))):
        d[1].wait_recv()
        l.wait_recv()
        outs[t][0][:, outs[t][1]] = (part[t, sp] + rd2[t] + rl[t]).astype(BF16)
    e2.wait()
    tot = er[1] + er[2]
    dg_out[...] = tot[0:1]
    db_out[...] = tot[1:2]
    d3[1].wait_recv()
    l3.wait_recv()
    outs[3][0][:, outs[3][1]] = (part[3, sp] + rd2[3] + rl[3]).astype(BF16)
    for copy in (a1, a2, b1, b2, c1, c2, *d0, *d1, *d2, *d3, l0, l1, l2, l3):
        copy.wait_send()


def local_step(x_rows, dy_rows, ln_gamma, ln_beta, w_qkv, w_out, temperature):
    any_spec = pl.BlockSpec(memory_space=pl.ANY)
    vmem = pl.BlockSpec(memory_space=pltpu.VMEM)
    smem = pl.BlockSpec(memory_space=pltpu.SMEM)
    sds = jax.ShapeDtypeStruct
    outs = pl.pallas_call(
        kernel,
        out_shape=(sds((N, D), BF16), sds((N, D), BF16), sds((RB, 3 * D), BF16), sds((RB, D), BF16),
                   sds((1, D), F32), sds((1, D), F32), sds((1, 8), F32)),
        in_specs=[any_spec, any_spec, vmem, vmem, any_spec, any_spec, smem],
        out_specs=(vmem,) * 7,
        scratch_shapes=[
            pltpu.VMEM((N, D), BF16),
            pltpu.VMEM((N, D), BF16),
            pltpu.VMEM((D, 3 * D), BF16),
            pltpu.VMEM((D, D), BF16),
            pltpu.VMEM((3 * D, D), BF16),
            pltpu.VMEM((N, D), BF16),
            pltpu.VMEM((D, N), BF16),
            pltpu.VMEM((3, 2, GW, N), BF16),
            pltpu.VMEM((3, 2, GW, N), BF16),
            pltpu.VMEM((2, GW, N), BF16),
            pltpu.VMEM((2, GW, N), BF16),
            pltpu.VMEM((N, 1), F32),
            pltpu.VMEM((N, 1), F32),
            pltpu.VMEM((2 * D, 128), F32),
            pltpu.VMEM((2, HD, PW), F32),
            pltpu.VMEM((2, HD, PW), F32),
            pltpu.VMEM((2, HD, PW), F32),
            pltpu.VMEM((2, HD, PW), F32),
            pltpu.VMEM((2, HD, PW), F32),
            pltpu.VMEM((2, HD, PW), F32),
            pltpu.VMEM((2, HD, PW), F32),
            pltpu.VMEM((2, GW, GW), BF16),
            pltpu.VMEM((2, GW, GW), BF16),
            pltpu.VMEM((6, HD, PW), F32),
            pltpu.VMEM((4, 4, RB, D), F32),
            pltpu.VMEM((4, RB, D), F32),
            pltpu.VMEM((4, RB, D), F32),
            pltpu.VMEM((4, RB, D), F32),
            pltpu.VMEM((4, RB, D), F32),
            pltpu.VMEM((8, D), F32),
            pltpu.VMEM((3, 8, D), F32),
            pltpu.SemaphoreType.DMA((3,)),
            pltpu.SemaphoreType.DMA((NCH,)),
            pltpu.SemaphoreType.DMA((20,)),
            pltpu.SemaphoreType.DMA((20,)),
        ],
        compiler_params=pltpu.CompilerParams(collective_id=0, has_side_effects=True, vmem_limit_bytes=48 << 20),
        name="xca",
    )(x_rows, dy_rows, ln_gamma.reshape(1, D), ln_beta.reshape(1, D), w_qkv, w_out, temperature)
    y, dx, dw, dwo, dg, db, dt = outs
    return y, dx, dw, dwo, dg.reshape(D), db.reshape(D), dt.reshape(8)


def solution(mesh):
    row_spec = P(('dp', 'sp'), None)
    full_mat = P(None, None)
    full_vec = P(None)
    part_vec = P('dp')
    return jax.shard_map(local_step, mesh=mesh,
                         in_specs=(row_spec, row_spec, full_vec, full_vec, full_mat, full_mat, full_vec),
                         out_specs=(row_spec, row_spec, row_spec, row_spec, part_vec, part_vec, part_vec),
                         check_vma=False)
```

```python
import jax
import jax.numpy as jnp
from jax import lax
from jax.experimental import pallas as pl
from jax.experimental.pallas import tpu as pltpu
from jax.sharding import PartitionSpec as P

LN_EPS = 1e-6
F32 = jnp.float32
BF16 = jnp.bfloat16
N = 2048
D = 384
HD = 48
GW = 192
PW = 256
RB = 96
CH = 256
NCH = N // CH

NN = (((1,), (0,)), ((), ()))
NT = (((1,), (1,)), ((), ()))
TN = (((0,), (0,)), ((), ()))


def mm(a, b, dims):
    return lax.dot_general(a, b, dims, preferred_element_type=F32)


def kernel(x_hbm, dy_hbm, gamma_hbm, beta_hbm, w_hbm, wo_hbm, temp_hbm,
           y_out, dx_out, dw_out, dwo_out, dg_out, db_out, dt_out,
           x, dy, w, wo, wt, u, ut, qkvt, dqkvt, dot_, ot, mean_s, rstd_s, s_acc,
           pk1, pk2, ra, sb, rb, cs, rc, abd, gbd, keep, part, rd1, rd2, ls, rl, es, er,
           gamma, beta, temp, in_sem, x_sem, ssem, rsem):
    sp = lax.axis_index("sp")
    core = lax.rem(sp, 2)
    peer = 1 - core
    partner = sp + 1 - 2 * core
    other = lax.rem(sp + 2, 4)
    cross = lax.rem(partner + 2, 4)

    barrier = pltpu.get_barrier_semaphore()
    for dev in (partner, other):
        pl.semaphore_signal(barrier, inc=1, device_id={"sp": dev}, device_id_type=pl.DeviceIdType.MESH)

    w_copy = pltpu.make_async_copy(w_hbm, w, in_sem.at[0])
    wo_copy = pltpu.make_async_copy(wo_hbm, wo, in_sem.at[1])
    dy_copy = pltpu.make_async_copy(dy_hbm, dy, in_sem.at[2])
    gamma_copy = pltpu.make_async_copy(gamma_hbm, gamma.at[0], in_sem.at[3])
    beta_copy = pltpu.make_async_copy(beta_hbm, beta.at[0], in_sem.at[4])
    temp_copy = pltpu.make_async_copy(temp_hbm, temp, in_sem.at[5])

    def x_copy(i):
        rows = pl.ds(i * CH, CH)
        return pltpu.make_async_copy(x_hbm.at[rows], x.at[rows], x_sem.at[i])

    x_copy(0).start()
    gamma_copy.start()
    beta_copy.start()
    w_copy.start()
    for i in range(1, NCH):
        x_copy(i).start()
    wo_copy.start()
    dy_copy.start()
    temp_copy.start()

    def send(slot, src, dst, dev):
        copy = pltpu.make_async_remote_copy(
            src_ref=src, dst_ref=dst, send_sem=ssem.at[slot], recv_sem=rsem.at[slot],
            device_id={"sp": dev}, device_id_type=pl.DeviceIdType.MESH)
        copy.start()
        return copy

    lane = lax.broadcasted_iota(jnp.int32, (HD, PW), 1)
    row = lax.broadcasted_iota(jnp.int32, (HD, PW), 0)
    heads = [(lane >= HD * h) & (lane < HD * h + HD) for h in range(4)]
    eyes = [lane == row + HD * h for h in range(4)]
    valid = lane < GW
    s_acc[...] = jnp.zeros_like(s_acc)
    pk1[...] = jnp.zeros_like(pk1)
    pk2[...] = jnp.zeros_like(pk2)

    def layer_norm(i):
        rows = pl.ds(pl.multiple_of(i * CH, CH), CH)
        xf = x[rows, :].astype(F32)
        mean = jnp.mean(xf, axis=-1, keepdims=True)
        cen = xf - mean
        rstd = lax.rsqrt(jnp.mean(cen * cen, axis=-1, keepdims=True) + LN_EPS)
        mean_s[rows, :] = mean
        rstd_s[rows, :] = rstd
        u[rows, :] = (cen * rstd * gamma[...] + beta[...]).astype(BF16)

    def qk_chunk(i):
        cols = pl.ds(pl.multiple_of(i * CH, CH), CH)
        res = mm(wt[0:2 * D, :], u[cols, :], NT).astype(BF16)
        for s in range(4):
            qkvt[s // 2, s % 2, :, cols] = res[s * GW:(s + 1) * GW]
        sq = jnp.square(res.astype(F32))
        s_acc[...] += sq[:, :128] + sq[:, 128:]

    gamma_copy.wait()
    beta_copy.wait()
    x_copy(0).wait()
    layer_norm(0)
    w_copy.wait()
    wt[...] = w[...].T

    @pl.loop(0, NCH - 1)
    def _(i):
        rows = pl.ds(pl.multiple_of((i + 1) * CH, CH), CH)
        pltpu.make_async_copy(x_hbm.at[rows], x.at[rows], x_sem.at[i + 1]).wait()
        qk_chunk(i)
        layer_norm(i + 1)

    qk_chunk(NCH - 1)

    def compact(full):
        out = jnp.zeros((HD, GW), F32)
        for h in range(4):
            out = jnp.where(heads[h][:, :GW], full[HD * h:HD * h + HD], out)
        return out

    s_col = jnp.sum(s_acc[...], axis=-1, keepdims=True)
    for g in range(2):
        pk1[g, :, 0:GW] = compact(mm(qkvt[0, g], qkvt[1, g], NT))
        blk = pk1[g]
        for h in range(4):
            r = g * GW + h * HD
            blk = jnp.where(lane == GW + h, s_col[r:r + HD], blk)
            blk = jnp.where(lane == GW + 4 + h, s_col[D + r:D + r + HD], blk)
        pk1[g] = blk

    pl.semaphore_wait(barrier, 2)
    a1 = send(0, pk1.at[peer], ra.at[0], partner)

    CV = 512

    @pl.loop(0, N // CV)
    def _(i):
        cols = pl.ds(pl.multiple_of(i * CV, CV), CV)
        res = mm(wt[2 * D:3 * D, :], u[cols, :], NT).astype(BF16)
        qkvt[2, 0, :, cols] = res[:GW]
        qkvt[2, 1, :, cols] = res[GW:]

    a1.wait_recv()
    sb[0] = pk1[core] + ra[0]
    b1 = send(1, sb.at[0], rb.at[0], other)

    wo_copy.wait()
    dy_copy.wait()
    temp_copy.wait()

    @pl.loop(0, N // CV)
    def _(i):
        cols = pl.ds(pl.multiple_of(i * CV, CV), CV)
        res = mm(wo[...], dy[cols, :], NT).astype(BF16)
        dot_[0, :, cols] = res[:GW]
        dot_[1, :, cols] = res[GW:]

    for g in range(2):
        pk2[g, :, 0:GW] = compact(mm(dot_[g], qkvt[2, g], NT))
    a2 = send(2, pk2.at[peer], ra.at[1], partner)

    @pl.loop(0, NCH // 2)
    def _(i):
        cols = pl.ds(pl.multiple_of(i * CH, CH), CH)
        ut[:, cols] = u[cols, :].T

    a2.wait_recv()
    sb[1] = pk2[core] + ra[1]
    b2 = send(3, sb.at[1], rb.at[1], other)

    @pl.loop(NCH // 2, NCH)
    def _(i):
        cols = pl.ds(pl.multiple_of(i * CH, CH), CH)
        ut[:, cols] = u[cols, :].T

    def seg_sum(v):
        out = jnp.zeros_like(v)
        for h in range(4):
            out = jnp.where(heads[h], jnp.sum(jnp.where(heads[h], v, 0.0), axis=-1, keepdims=True), out)
        return out

    def expand(dst, g, comp):
        for h in range(4):
            dst[g, HD * h:HD * h + HD, :] = jnp.where(heads[h], comp, 0.0)[:, :GW].astype(BF16)

    b1.wait_recv()
    gs = sb[0] + rb[0]
    rq2 = jnp.zeros((HD, PW), F32)
    rk2 = jnp.zeros((HD, PW), F32)
    tau = jnp.zeros((HD, PW), F32)
    for h in range(4):
        sq_h = jnp.sum(jnp.where(lane == GW + h, gs, 0.0), axis=-1, keepdims=True)
        sk_h = jnp.sum(jnp.where(lane == GW + 4 + h, gs, 0.0), axis=-1, keepdims=True)
        rq2 = jnp.where(heads[h], sq_h, rq2)
        rk2 = jnp.where(eyes[h], sk_h, rk2)
        tau = jnp.where(heads[h], temp[core * 4 + h], tau)
    sk2 = jnp.sum(rk2, axis=0, keepdims=True)
    q_inv = lax.rsqrt(jnp.where(valid, rq2, 1.0))
    k_inv = lax.rsqrt(jnp.where(valid, sk2, 1.0))
    gram = jnp.where(valid, gs, 0.0)
    scores = tau * gram * q_inv * k_inv
    top = jnp.zeros((HD, PW), F32)
    for h in range(4):
        top = jnp.where(heads[h], jnp.max(jnp.where(heads[h], scores, -jnp.inf), axis=-1, keepdims=True), top)
    e = jnp.where(valid, jnp.exp(scores - top), 0.0)
    prob = jnp.where(valid, e / jnp.where(valid, seg_sum(e), 1.0), 0.0)
    cs[0] = prob
    c1 = send(4, cs.at[0], rc.at[0], partner)
    keep[0] = prob
    keep[1] = scores
    keep[2] = gram * q_inv * k_inv
    keep[3] = tau * q_inv * k_inv
    keep[4] = jnp.where(valid, rq2, 1.0)
    keep[5] = jnp.where(valid, jnp.broadcast_to(sk2, (HD, PW)), 1.0)
    expand(abd, core, prob)

    def attend(g):
        ot[g] = mm(abd[g], qkvt[2, g], NN).astype(BF16)

    def d_value(g):
        dqkvt[2, g] = mm(abd[g], dot_[g], TN).astype(BF16)

    attend(core)
    d_value(core)
    c1.wait_recv()
    expand(abd, peer, rc[0])
    attend(peer)

    def all_rows(ref):
        return ref[...].reshape(D, N)

    def weight_send(t):
        return (send(6 + 3 * t, part.at[t, cross], rd1.at[t], partner),
                send(7 + 3 * t, part.at[t, partner], rd2.at[t], partner))

    def link_send(t, first):
        first.wait_recv()
        ls[t] = part[t, other] + rd1[t]
        return send(8 + 3 * t, ls.at[t], rl.at[t], other)

    part[0] = mm(all_rows(ot), dy[...], NN).reshape(4, RB, D)
    d0 = weight_send(0)

    b2.wait_recv()
    da = jnp.where(valid, (sb[1] + rb[1]).astype(BF16).astype(F32), 0.0)
    p = keep[0]
    ds = p * (da - seg_sum(da * p))
    weighted = ds * keep[1]
    dtemp = seg_sum(ds * keep[2])
    dtemp = jnp.sum(dtemp, axis=0, keepdims=True)
    dgram = (ds * keep[3]).astype(BF16).astype(F32)
    dsq = -seg_sum(weighted) / keep[4]
    dsk = -jnp.sum(weighted, axis=0, keepdims=True) / keep[5]
    blk = dgram
    for h in range(4):
        dsk_h = jnp.sum(jnp.where(eyes[h], dsk, 0.0), axis=-1, keepdims=True)
        dsq_h = jnp.sum(jnp.where(eyes[h], dsq, 0.0), axis=-1, keepdims=True)
        dt_h = jnp.sum(jnp.where(lane == HD * h, dtemp, 0.0), axis=-1, keepdims=True)
        blk = jnp.where(lane == GW + h, dsq_h, blk)
        blk = jnp.where(lane == GW + 4 + h, dsk_h, blk)
        blk = jnp.where(lane == GW + 8 + h, dt_h, blk)
    cs[1] = blk
    c2 = send(5, cs.at[1], rc.at[1], partner)

    l0 = link_send(0, d0[0])

    d_value(peer)
    part[1] = mm(all_rows(ut), dqkvt[2].reshape(D, N), NT).reshape(4, RB, D)
    d1 = weight_send(1)

    def d_qk(g, blk):
        expand(gbd, g, jnp.where(valid, blk, 0.0))
        cols = []
        for b in (GW, GW + 4):
            cols.append(jnp.concatenate(
                [jnp.sum(jnp.where(lane == b + h, blk, 0.0), axis=-1, keepdims=True) for h in range(4)], axis=0))
        dqkvt[0, g] = (mm(gbd[g], qkvt[1, g], NN) + qkvt[0, g].astype(F32) * cols[0]).astype(BF16)
        dqkvt[1, g] = (mm(gbd[g], qkvt[0, g], TN) + qkvt[1, g].astype(F32) * cols[1]).astype(BF16)

    d_qk(core, cs[1])
    c2.wait_recv()
    d_qk(peer, rc[1])
    l1 = link_send(1, d1[0])
    part[2] = mm(ut[...], dqkvt[1].reshape(D, N), NT).reshape(4, RB, D)
    d2 = weight_send(2)
    part[3] = mm(ut[...], dqkvt[0].reshape(D, N), NT).reshape(4, RB, D)
    d3 = weight_send(3)
    l2 = link_send(2, d2[0])
    l3 = link_send(3, d3[0])

    lane8 = lax.broadcasted_iota(jnp.int32, (1, 8), 1)
    dt = jnp.zeros((1, 8), F32)
    for g, src in ((core, cs), (peer, rc)):
        head_row = src[1][0:1, :]
        for h in range(4):
            val = jnp.sum(jnp.where(lane[0:1] == GW + 8 + h, head_row, 0.0), axis=-1, keepdims=True)
            dt = jnp.where(lane8 == g * 4 + h, val, dt)
    dt_out[...] = dt

    es[...] = jnp.zeros_like(es)

    @pl.loop(0, NCH)
    def _(i):
        rows = pl.ds(pl.multiple_of(i * CH, CH), CH)
        proj = mm(ot[:, :, rows].reshape(D, CH), wo[...], TN)
        xf = x[rows, :].astype(F32)
        y_out[rows, :] = (xf + proj).astype(BF16)
        dut = mm(w[...], dqkvt[:, :, :, rows].reshape(3 * D, CH), NN).astype(BF16)
        du = dut.T.astype(F32)
        rstd = rstd_s[rows, :]
        xhat = (xf - mean_s[rows, :]) * rstd
        es[0:1, :] += jnp.sum(du * xhat, axis=0, keepdims=True)
        es[1:2, :] += jnp.sum(du, axis=0, keepdims=True)
        dh = du * gamma[...]
        m1 = jnp.mean(dh, axis=-1, keepdims=True)
        m2 = jnp.mean(dh * xhat, axis=-1, keepdims=True)
        dx_out[rows, :] = (dy[rows, :].astype(F32) + rstd * (dh - m1 - xhat * m2)).astype(BF16)

    e1 = send(18, es, er.at[0], partner)
    e1.wait()
    er[1] = es[...] + er[0]
    e2 = send(19, er.at[1], er.at[2], other)

    outs = ((dwo_out, slice(0, D)), (dw_out, slice(2 * D, 3 * D)), (dw_out, slice(D, 2 * D)), (dw_out, slice(0, D)))
    for t, (d, l) in enumerate(((d0, l0), (d1, l1), (d2, l2))):
        d[1].wait_recv()
        l.wait_recv()
        outs[t][0][:, outs[t][1]] = (part[t, sp] + rd2[t] + rl[t]).astype(BF16)
    e2.wait()
    tot = er[1] + er[2]
    dg_out[...] = tot[0:1]
    db_out[...] = tot[1:2]
    d3[1].wait_recv()
    l3.wait_recv()
    outs[3][0][:, outs[3][1]] = (part[3, sp] + rd2[3] + rl[3]).astype(BF16)
    for copy in (a1, a2, b1, b2, c1, c2, *d0, *d1, *d2, *d3, l0, l1, l2, l3):
        copy.wait_send()


def write_out(y, dx, dw, dwo, dg, db, dt, y_o, dx_o, dw_o, dwo_o, dg_o, db_o, dt_o, sem):
    copies = [pltpu.make_async_copy(src, dst, sem.at[i]) for i, (src, dst) in enumerate(
        ((y, y_o), (dx, dx_o), (dw, dw_o), (dwo, dwo_o), (dg.at[0], dg_o), (db.at[0], db_o), (dt.at[0], dt_o)))]
    for copy in copies:
        copy.start()
    for copy in copies:
        copy.wait()


def local_step(x_rows, dy_rows, ln_gamma, ln_beta, w_qkv, w_out, temperature):
    hbm = pl.BlockSpec(memory_space=pltpu.HBM)
    vmem = pl.BlockSpec(memory_space=pltpu.VMEM)
    sds = jax.ShapeDtypeStruct
    outs = pl.pallas_call(
        kernel,
        out_shape=(sds((N, D), BF16), sds((N, D), BF16), sds((RB, 3 * D), BF16), sds((RB, D), BF16),
                   sds((1, D), F32), sds((1, D), F32), sds((1, 8), F32)),
        in_specs=[hbm] * 7,
        out_specs=(vmem,) * 7,
        scratch_shapes=[
            pltpu.VMEM((N, D), BF16),
            pltpu.VMEM((N, D), BF16),
            pltpu.VMEM((D, 3 * D), BF16),
            pltpu.VMEM((D, D), BF16),
            pltpu.VMEM((3 * D, D), BF16),
            pltpu.VMEM((N, D), BF16),
            pltpu.VMEM((D, N), BF16),
            pltpu.VMEM((3, 2, GW, N), BF16),
            pltpu.VMEM((3, 2, GW, N), BF16),
            pltpu.VMEM((2, GW, N), BF16),
            pltpu.VMEM((2, GW, N), BF16),
            pltpu.VMEM((N, 1), F32),
            pltpu.VMEM((N, 1), F32),
            pltpu.VMEM((2 * D, 128), F32),
            pltpu.VMEM((2, HD, PW), F32),
            pltpu.VMEM((2, HD, PW), F32),
            pltpu.VMEM((2, HD, PW), F32),
            pltpu.VMEM((2, HD, PW), F32),
            pltpu.VMEM((2, HD, PW), F32),
            pltpu.VMEM((2, HD, PW), F32),
            pltpu.VMEM((2, HD, PW), F32),
            pltpu.VMEM((2, GW, GW), BF16),
            pltpu.VMEM((2, GW, GW), BF16),
            pltpu.VMEM((6, HD, PW), F32),
            pltpu.VMEM((4, 4, RB, D), F32),
            pltpu.VMEM((4, RB, D), F32),
            pltpu.VMEM((4, RB, D), F32),
            pltpu.VMEM((4, RB, D), F32),
            pltpu.VMEM((4, RB, D), F32),
            pltpu.VMEM((8, D), F32),
            pltpu.VMEM((3, 8, D), F32),
            pltpu.VMEM((1, D), F32),
            pltpu.VMEM((1, D), F32),
            pltpu.SMEM((8,), F32),
            pltpu.SemaphoreType.DMA((6,)),
            pltpu.SemaphoreType.DMA((NCH,)),
            pltpu.SemaphoreType.DMA((20,)),
            pltpu.SemaphoreType.DMA((20,)),
        ],
        compiler_params=pltpu.CompilerParams(collective_id=0, has_side_effects=True, vmem_limit_bytes=48 << 20),
        name="xca",
    )(x_rows, dy_rows, ln_gamma, ln_beta, w_qkv, w_out, temperature)
    return pl.pallas_call(
        write_out,
        out_shape=(sds((N, D), BF16), sds((N, D), BF16), sds((RB, 3 * D), BF16), sds((RB, D), BF16),
                   sds((D,), F32), sds((D,), F32), sds((8,), F32)),
        in_specs=[vmem] * 7,
        out_specs=(hbm,) * 7,
        scratch_shapes=[pltpu.SemaphoreType.DMA((7,))],
        name="write_out",
    )(*outs)


def solution(mesh):
    row_spec = P(('dp', 'sp'), None)
    full_mat = P(None, None)
    full_vec = P(None)
    part_vec = P('dp')
    return jax.shard_map(local_step, mesh=mesh,
                         in_specs=(row_spec, row_spec, full_vec, full_vec, full_mat, full_mat, full_vec),
                         out_specs=(row_spec, row_spec, row_spec, row_spec, part_vec, part_vec, part_vec),
                         check_vma=False)
```

```python
import jax
import jax.numpy as jnp
from jax import lax
from jax.experimental import pallas as pl
from jax.experimental.pallas import tpu as pltpu
from jax.sharding import PartitionSpec as P

LN_EPS = 1e-6
F32 = jnp.float32
BF16 = jnp.bfloat16
N = 2048
D = 384
HD = 48
GW = 192
PW = 256
RB = 96
CH = 256
NCH = N // CH

NN = (((1,), (0,)), ((), ()))
NT = (((1,), (1,)), ((), ()))
TN = (((0,), (0,)), ((), ()))


def mm(a, b, dims):
    return lax.dot_general(a, b, dims, preferred_element_type=F32)


def kernel(x_hbm, dy_hbm, gamma_hbm, beta_hbm, w_hbm, wo_hbm, temp_hbm,
           y_out, dx_out, dw_out, dwo_out, dg_out, db_out, dt_out,
           x, dy, w, wo, wt, u, ut, qkvt, dqkvt, dot_, ot, mean_s, rstd_s, s_acc,
           pk1, pk2, ra, sb, rb, cs, rc, abd, gbd, keep, part, rd1, rd2, ls, rl, es, er,
           gamma, beta, temp, in_sem, x_sem, ssem, rsem):
    sp = lax.axis_index("sp")
    core = lax.rem(sp, 2)
    peer = 1 - core
    partner = sp + 1 - 2 * core
    other = lax.rem(sp + 2, 4)
    cross = lax.rem(partner + 2, 4)

    barrier = pltpu.get_barrier_semaphore()
    for dev in (partner, other):
        pl.semaphore_signal(barrier, inc=1, device_id={"sp": dev}, device_id_type=pl.DeviceIdType.MESH)

    w_copy = pltpu.make_async_copy(w_hbm, w, in_sem.at[0])
    wo_copy = pltpu.make_async_copy(wo_hbm, wo, in_sem.at[1])
    dy_copy = pltpu.make_async_copy(dy_hbm, dy, in_sem.at[2])
    gamma_copy = pltpu.make_async_copy(gamma_hbm, gamma.at[0], in_sem.at[3])
    beta_copy = pltpu.make_async_copy(beta_hbm, beta.at[0], in_sem.at[4])
    temp_copy = pltpu.make_async_copy(temp_hbm, temp, in_sem.at[5])

    def x_copy(i):
        rows = pl.ds(i * CH, CH)
        return pltpu.make_async_copy(x_hbm.at[rows], x.at[rows], x_sem.at[i])

    x_copy(0).start()
    gamma_copy.start()
    beta_copy.start()
    w_copy.start()
    for i in range(1, NCH):
        x_copy(i).start()
    wo_copy.start()
    dy_copy.start()
    temp_copy.start()

    def send(slot, src, dst, dev):
        copy = pltpu.make_async_remote_copy(
            src_ref=src, dst_ref=dst, send_sem=ssem.at[slot], recv_sem=rsem.at[slot],
            device_id={"sp": dev}, device_id_type=pl.DeviceIdType.MESH)
        copy.start()
        return copy

    lane = lax.broadcasted_iota(jnp.int32, (HD, PW), 1)
    row = lax.broadcasted_iota(jnp.int32, (HD, PW), 0)
    heads = [(lane >= HD * h) & (lane < HD * h + HD) for h in range(4)]
    eyes = [lane == row + HD * h for h in range(4)]
    valid = lane < GW
    s_acc[...] = jnp.zeros_like(s_acc)
    pk1[...] = jnp.zeros_like(pk1)
    pk2[...] = jnp.zeros_like(pk2)

    def layer_norm(i):
        rows = pl.ds(pl.multiple_of(i * CH, CH), CH)
        xf = x[rows, :].astype(F32)
        mean = jnp.mean(xf, axis=-1, keepdims=True)
        cen = xf - mean
        rstd = lax.rsqrt(jnp.mean(cen * cen, axis=-1, keepdims=True) + LN_EPS)
        mean_s[rows, :] = mean
        rstd_s[rows, :] = rstd
        u[rows, :] = (cen * rstd * gamma[...] + beta[...]).astype(BF16)

    def qk_chunk(i):
        cols = pl.ds(pl.multiple_of(i * CH, CH), CH)
        res = mm(wt[0:2 * D, :], u[cols, :], NT).astype(BF16)
        for s in range(4):
            qkvt[s // 2, s % 2, :, cols] = res[s * GW:(s + 1) * GW]
        sq = jnp.square(res.astype(F32))
        s_acc[...] += sq[:, :128] + sq[:, 128:]

    gamma_copy.wait()
    beta_copy.wait()
    x_copy(0).wait()
    layer_norm(0)
    w_copy.wait()
    wt[...] = w[...].T

    @pl.loop(0, NCH - 1)
    def _(i):
        rows = pl.ds(pl.multiple_of((i + 1) * CH, CH), CH)
        pltpu.make_async_copy(x_hbm.at[rows], x.at[rows], x_sem.at[i + 1]).wait()
        qk_chunk(i)
        layer_norm(i + 1)

    qk_chunk(NCH - 1)

    def compact(full):
        out = jnp.zeros((HD, GW), F32)
        for h in range(4):
            out = jnp.where(heads[h][:, :GW], full[HD * h:HD * h + HD], out)
        return out

    s_col = jnp.sum(s_acc[...], axis=-1, keepdims=True)
    for g in range(2):
        pk1[g, :, 0:GW] = compact(mm(qkvt[0, g], qkvt[1, g], NT))
        blk = pk1[g]
        for h in range(4):
            r = g * GW + h * HD
            blk = jnp.where(lane == GW + h, s_col[r:r + HD], blk)
            blk = jnp.where(lane == GW + 4 + h, s_col[D + r:D + r + HD], blk)
        pk1[g] = blk

    pl.semaphore_wait(barrier, 2)
    a1 = send(0, pk1.at[peer], ra.at[0], partner)

    CV = 512

    @pl.loop(0, N // CV)
    def _(i):
        cols = pl.ds(pl.multiple_of(i * CV, CV), CV)
        res = mm(wt[2 * D:3 * D, :], u[cols, :], NT).astype(BF16)
        qkvt[2, 0, :, cols] = res[:GW]
        qkvt[2, 1, :, cols] = res[GW:]

    a1.wait_recv()
    sb[0] = pk1[core] + ra[0]
    b1 = send(1, sb.at[0], rb.at[0], other)

    wo_copy.wait()
    dy_copy.wait()
    temp_copy.wait()

    @pl.loop(0, N // CV)
    def _(i):
        cols = pl.ds(pl.multiple_of(i * CV, CV), CV)
        res = mm(wo[...], dy[cols, :], NT).astype(BF16)
        dot_[0, :, cols] = res[:GW]
        dot_[1, :, cols] = res[GW:]

    for g in range(2):
        pk2[g, :, 0:GW] = compact(mm(dot_[g], qkvt[2, g], NT))
    a2 = send(2, pk2.at[peer], ra.at[1], partner)

    @pl.loop(0, NCH // 2)
    def _(i):
        cols = pl.ds(pl.multiple_of(i * CH, CH), CH)
        ut[:, cols] = u[cols, :].T

    a2.wait_recv()
    sb[1] = pk2[core] + ra[1]
    b2 = send(3, sb.at[1], rb.at[1], other)

    @pl.loop(NCH // 2, NCH)
    def _(i):
        cols = pl.ds(pl.multiple_of(i * CH, CH), CH)
        ut[:, cols] = u[cols, :].T

    def seg_sum(v):
        out = jnp.zeros_like(v)
        for h in range(4):
            out = jnp.where(heads[h], jnp.sum(jnp.where(heads[h], v, 0.0), axis=-1, keepdims=True), out)
        return out

    def expand(dst, g, comp):
        for h in range(4):
            dst[g, HD * h:HD * h + HD, :] = jnp.where(heads[h], comp, 0.0)[:, :GW].astype(BF16)

    b1.wait_recv()
    gs = sb[0] + rb[0]
    rq2 = jnp.zeros((HD, PW), F32)
    rk2 = jnp.zeros((HD, PW), F32)
    tau = jnp.zeros((HD, PW), F32)
    for h in range(4):
        sq_h = jnp.sum(jnp.where(lane == GW + h, gs, 0.0), axis=-1, keepdims=True)
        sk_h = jnp.sum(jnp.where(lane == GW + 4 + h, gs, 0.0), axis=-1, keepdims=True)
        rq2 = jnp.where(heads[h], sq_h, rq2)
        rk2 = jnp.where(eyes[h], sk_h, rk2)
        tau = jnp.where(heads[h], temp[core * 4 + h], tau)
    sk2 = jnp.sum(rk2, axis=0, keepdims=True)
    q_inv = lax.rsqrt(jnp.where(valid, rq2, 1.0))
    k_inv = lax.rsqrt(jnp.where(valid, sk2, 1.0))
    gram = jnp.where(valid, gs, 0.0)
    scores = tau * gram * q_inv * k_inv
    top = jnp.zeros((HD, PW), F32)
    for h in range(4):
        top = jnp.where(heads[h], jnp.max(jnp.where(heads[h], scores, -jnp.inf), axis=-1, keepdims=True), top)
    e = jnp.where(valid, jnp.exp(scores - top), 0.0)
    prob = jnp.where(valid, e / jnp.where(valid, seg_sum(e), 1.0), 0.0)
    cs[0] = prob
    c1 = send(4, cs.at[0], rc.at[0], partner)
    keep[0] = prob
    keep[1] = scores
    keep[2] = gram * q_inv * k_inv
    keep[3] = tau * q_inv * k_inv
    keep[4] = jnp.where(valid, rq2, 1.0)
    keep[5] = jnp.where(valid, jnp.broadcast_to(sk2, (HD, PW)), 1.0)
    expand(abd, core, prob)

    def attend(g):
        ot[g] = mm(abd[g], qkvt[2, g], NN).astype(BF16)

    def d_value(g):
        dqkvt[2, g] = mm(abd[g], dot_[g], TN).astype(BF16)

    attend(core)
    d_value(core)
    c1.wait_recv()
    expand(abd, peer, rc[0])
    attend(peer)

    def all_rows(ref):
        return ref[...].reshape(D, N)

    def weight_send(t):
        return (send(6 + 3 * t, part.at[t, cross], rd1.at[t], partner),
                send(7 + 3 * t, part.at[t, partner], rd2.at[t], partner))

    def link_send(t, first):
        first.wait_recv()
        ls[t] = part[t, other] + rd1[t]
        return send(8 + 3 * t, ls.at[t], rl.at[t], other)

    part[0] = mm(all_rows(ot), dy[...], NN).reshape(4, RB, D)
    d0 = weight_send(0)

    b2.wait_recv()
    da = jnp.where(valid, (sb[1] + rb[1]).astype(BF16).astype(F32), 0.0)
    p = keep[0]
    ds = p * (da - seg_sum(da * p))
    weighted = ds * keep[1]
    dtemp = seg_sum(ds * keep[2])
    dtemp = jnp.sum(dtemp, axis=0, keepdims=True)
    dgram = (ds * keep[3]).astype(BF16).astype(F32)
    dsq = -seg_sum(weighted) / keep[4]
    dsk = -jnp.sum(weighted, axis=0, keepdims=True) / keep[5]
    blk = dgram
    for h in range(4):
        dsk_h = jnp.sum(jnp.where(eyes[h], dsk, 0.0), axis=-1, keepdims=True)
        dsq_h = jnp.sum(jnp.where(eyes[h], dsq, 0.0), axis=-1, keepdims=True)
        dt_h = jnp.sum(jnp.where(lane == HD * h, dtemp, 0.0), axis=-1, keepdims=True)
        blk = jnp.where(lane == GW + h, dsq_h, blk)
        blk = jnp.where(lane == GW + 4 + h, dsk_h, blk)
        blk = jnp.where(lane == GW + 8 + h, dt_h, blk)
    cs[1] = blk
    c2 = send(5, cs.at[1], rc.at[1], partner)

    l0 = link_send(0, d0[0])

    d_value(peer)
    part[1] = mm(all_rows(ut), dqkvt[2].reshape(D, N), NT).reshape(4, RB, D)
    d1 = weight_send(1)

    def d_qk(g, blk):
        expand(gbd, g, jnp.where(valid, blk, 0.0))
        cols = []
        for b in (GW, GW + 4):
            cols.append(jnp.concatenate(
                [jnp.sum(jnp.where(lane == b + h, blk, 0.0), axis=-1, keepdims=True) for h in range(4)], axis=0))
        dqkvt[0, g] = (mm(gbd[g], qkvt[1, g], NN) + qkvt[0, g].astype(F32) * cols[0]).astype(BF16)
        dqkvt[1, g] = (mm(gbd[g], qkvt[0, g], TN) + qkvt[1, g].astype(F32) * cols[1]).astype(BF16)

    d_qk(core, cs[1])
    c2.wait_recv()
    d_qk(peer, rc[1])
    l1 = link_send(1, d1[0])
    part[2] = mm(ut[...], dqkvt[1].reshape(D, N), NT).reshape(4, RB, D)
    d2 = weight_send(2)
    part[3] = mm(ut[...], dqkvt[0].reshape(D, N), NT).reshape(4, RB, D)
    d3 = weight_send(3)
    l2 = link_send(2, d2[0])
    l3 = link_send(3, d3[0])

    lane8 = lax.broadcasted_iota(jnp.int32, (1, 8), 1)
    dt = jnp.zeros((1, 8), F32)
    for g, src in ((core, cs), (peer, rc)):
        head_row = src[1][0:1, :]
        for h in range(4):
            val = jnp.sum(jnp.where(lane[0:1] == GW + 8 + h, head_row, 0.0), axis=-1, keepdims=True)
            dt = jnp.where(lane8 == g * 4 + h, val, dt)
    dt_out[...] = dt

    es[...] = jnp.zeros_like(es)

    @pl.loop(0, NCH)
    def _(i):
        rows = pl.ds(pl.multiple_of(i * CH, CH), CH)
        proj = mm(ot[:, :, rows].reshape(D, CH), wo[...], TN)
        xf = x[rows, :].astype(F32)
        y_out[rows, :] = (xf + proj).astype(BF16)
        dut = mm(w[...], dqkvt[:, :, :, rows].reshape(3 * D, CH), NN).astype(BF16)
        du = dut.T.astype(F32)
        rstd = rstd_s[rows, :]
        xhat = (xf - mean_s[rows, :]) * rstd
        es[0:1, :] += jnp.sum(du * xhat, axis=0, keepdims=True)
        es[1:2, :] += jnp.sum(du, axis=0, keepdims=True)
        dh = du * gamma[...]
        m1 = jnp.mean(dh, axis=-1, keepdims=True)
        m2 = jnp.mean(dh * xhat, axis=-1, keepdims=True)
        dx_out[rows, :] = (dy[rows, :].astype(F32) + rstd * (dh - m1 - xhat * m2)).astype(BF16)

    e1 = send(18, es, er.at[0], partner)
    e1.wait()
    er[1] = es[...] + er[0]
    e2 = send(19, er.at[1], er.at[2], other)

    outs = ((dwo_out, slice(0, D)), (dw_out, slice(2 * D, 3 * D)), (dw_out, slice(D, 2 * D)), (dw_out, slice(0, D)))
    for t, (d, l) in enumerate(((d0, l0), (d1, l1), (d2, l2))):
        d[1].wait_recv()
        l.wait_recv()
        outs[t][0][:, outs[t][1]] = (part[t, sp] + rd2[t] + rl[t]).astype(BF16)
    e2.wait()
    tot = er[1] + er[2]
    dg_out[...] = tot[0:1]
    db_out[...] = tot[1:2]
    d3[1].wait_recv()
    l3.wait_recv()
    outs[3][0][:, outs[3][1]] = (part[3, sp] + rd2[3] + rl[3]).astype(BF16)
    for copy in (a1, a2, b1, b2, c1, c2, *d0, *d1, *d2, *d3, l0, l1, l2, l3):
        copy.wait_send()


def write_out(y, dx, dw, dwo, dg, db, dt, y_o, dx_o, dw_o, dwo_o, dg_o, db_o, dt_o, sem):
    copies = [pltpu.make_async_copy(src, dst, sem.at[i]) for i, (src, dst) in enumerate(
        ((y, y_o), (dx, dx_o), (dw, dw_o), (dwo, dwo_o), (dg.at[0], dg_o), (db.at[0], db_o), (dt.at[0], dt_o)))]
    for copy in copies:
        copy.start()
    for copy in copies:
        copy.wait()


def local_step(x_rows, dy_rows, ln_gamma, ln_beta, w_qkv, w_out, temperature):
    hbm = pl.BlockSpec(memory_space=pltpu.HBM)
    vmem = pl.BlockSpec(memory_space=pltpu.VMEM)
    sds = jax.ShapeDtypeStruct
    outs = pl.pallas_call(
        kernel,
        out_shape=(sds((N, D), BF16), sds((N, D), BF16), sds((RB, 3 * D), BF16), sds((RB, D), BF16),
                   sds((1, D), F32), sds((1, D), F32), sds((1, 8), F32)),
        in_specs=[hbm] * 7,
        out_specs=(vmem,) * 7,
        scratch_shapes=[
            pltpu.VMEM((N, D), BF16),
            pltpu.VMEM((N, D), BF16),
            pltpu.VMEM((D, 3 * D), BF16),
            pltpu.VMEM((D, D), BF16),
            pltpu.VMEM((3 * D, D), BF16),
            pltpu.VMEM((N, D), BF16),
            pltpu.VMEM((D, N), BF16),
            pltpu.VMEM((3, 2, GW, N), BF16),
            pltpu.VMEM((3, 2, GW, N), BF16),
            pltpu.VMEM((2, GW, N), BF16),
            pltpu.VMEM((2, GW, N), BF16),
            pltpu.VMEM((N, 1), F32),
            pltpu.VMEM((N, 1), F32),
            pltpu.VMEM((2 * D, 128), F32),
            pltpu.VMEM((2, HD, PW), F32),
            pltpu.VMEM((2, HD, PW), F32),
            pltpu.VMEM((2, HD, PW), F32),
            pltpu.VMEM((2, HD, PW), F32),
            pltpu.VMEM((2, HD, PW), F32),
            pltpu.VMEM((2, HD, PW), F32),
            pltpu.VMEM((2, HD, PW), F32),
            pltpu.VMEM((2, GW, GW), BF16),
            pltpu.VMEM((2, GW, GW), BF16),
            pltpu.VMEM((6, HD, PW), F32),
            pltpu.VMEM((4, 4, RB, D), F32),
            pltpu.VMEM((4, RB, D), F32),
            pltpu.VMEM((4, RB, D), F32),
            pltpu.VMEM((4, RB, D), F32),
            pltpu.VMEM((4, RB, D), F32),
            pltpu.VMEM((8, D), F32),
            pltpu.VMEM((3, 8, D), F32),
            pltpu.VMEM((1, D), F32),
            pltpu.VMEM((1, D), F32),
            pltpu.SMEM((8,), F32),
            pltpu.SemaphoreType.DMA((6,)),
            pltpu.SemaphoreType.DMA((NCH,)),
            pltpu.SemaphoreType.DMA((20,)),
            pltpu.SemaphoreType.DMA((20,)),
        ],
        compiler_params=pltpu.CompilerParams(collective_id=0, has_side_effects=True, vmem_limit_bytes=48 << 20),
        name="xca",
    )(*(pltpu.with_memory_space_constraint(a, pltpu.HBM)
        for a in (x_rows, dy_rows, ln_gamma, ln_beta, w_qkv, w_out, temperature)))
    return pl.pallas_call(
        write_out,
        out_shape=(sds((N, D), BF16), sds((N, D), BF16), sds((RB, 3 * D), BF16), sds((RB, D), BF16),
                   sds((D,), F32), sds((D,), F32), sds((8,), F32)),
        in_specs=[pl.BlockSpec(memory_space=pl.ANY)] * 7,
        out_specs=(hbm,) * 7,
        scratch_shapes=[pltpu.SemaphoreType.DMA((7,))],
        compiler_params=pltpu.CompilerParams(vmem_limit_bytes=1 << 20),
        name="write_out",
    )(*outs)


def solution(mesh):
    row_spec = P(('dp', 'sp'), None)
    full_mat = P(None, None)
    full_vec = P(None)
    part_vec = P('dp')
    return jax.shard_map(local_step, mesh=mesh,
                         in_specs=(row_spec, row_spec, full_vec, full_vec, full_mat, full_mat, full_vec),
                         out_specs=(row_spec, row_spec, row_spec, row_spec, part_vec, part_vec, part_vec),
                         check_vma=False)
```

```python
import jax
import jax.numpy as jnp
from jax import lax
from jax.experimental import pallas as pl
from jax.experimental.pallas import tpu as pltpu
from jax.sharding import PartitionSpec as P

LN_EPS = 1e-6
F32 = jnp.float32
BF16 = jnp.bfloat16
N = 2048
D = 384
HD = 48
GW = 192
PW = 256
RB = 96
CH = 512
NCH = N // CH

NN = (((1,), (0,)), ((), ()))
NT = (((1,), (1,)), ((), ()))
TN = (((0,), (0,)), ((), ()))


def mm(a, b, dims):
    return lax.dot_general(a, b, dims, preferred_element_type=F32)


def kernel(x_hbm, dy_hbm, gamma_hbm, beta_hbm, w_hbm, wo_hbm, temp_hbm,
           y_out, dx_out, dw_out, dwo_out, dg_out, db_out, dt_out,
           x, dy, w, wo, wt, u, ut, qkvt, dqkvt, dot_, ot, mean_s, rstd_s, s_acc,
           pk1, pk2, ra, sb, rb, cs, rc, abd, gbd, keep, part, rd1, rd2, ls, rl, es, er,
           gamma, beta, temp, in_sem, x_sem, ssem, rsem):
    sp = lax.axis_index("sp")
    core = lax.rem(sp, 2)
    peer = 1 - core
    partner = sp + 1 - 2 * core
    other = lax.rem(sp + 2, 4)
    cross = lax.rem(partner + 2, 4)

    barrier = pltpu.get_barrier_semaphore()
    for dev in (partner, other):
        pl.semaphore_signal(barrier, inc=1, device_id={"sp": dev}, device_id_type=pl.DeviceIdType.MESH)

    w_copy = pltpu.make_async_copy(w_hbm, w, in_sem.at[0])
    wo_copy = pltpu.make_async_copy(wo_hbm, wo, in_sem.at[1])
    dy_copy = pltpu.make_async_copy(dy_hbm, dy, in_sem.at[2])
    gamma_copy = pltpu.make_async_copy(gamma_hbm, gamma.at[0], in_sem.at[3])
    beta_copy = pltpu.make_async_copy(beta_hbm, beta.at[0], in_sem.at[4])
    temp_copy = pltpu.make_async_copy(temp_hbm, temp, in_sem.at[5])

    def x_copy(i):
        rows = pl.ds(i * CH, CH)
        return pltpu.make_async_copy(x_hbm.at[rows], x.at[rows], x_sem.at[i])

    x_copy(0).start()
    gamma_copy.start()
    beta_copy.start()
    w_copy.start()
    for i in range(1, NCH):
        x_copy(i).start()
    wo_copy.start()
    dy_copy.start()
    temp_copy.start()

    def send(slot, src, dst, dev):
        copy = pltpu.make_async_remote_copy(
            src_ref=src, dst_ref=dst, send_sem=ssem.at[slot], recv_sem=rsem.at[slot],
            device_id={"sp": dev}, device_id_type=pl.DeviceIdType.MESH)
        copy.start()
        return copy

    lane = lax.broadcasted_iota(jnp.int32, (HD, PW), 1)
    row = lax.broadcasted_iota(jnp.int32, (HD, PW), 0)
    heads = [(lane >= HD * h) & (lane < HD * h + HD) for h in range(4)]
    eyes = [lane == row + HD * h for h in range(4)]
    valid = lane < GW
    s_acc[...] = jnp.zeros_like(s_acc)
    pk1[...] = jnp.zeros_like(pk1)
    pk2[...] = jnp.zeros_like(pk2)
    es[...] = jnp.zeros_like(es)

    def layer_norm(i):
        rows = pl.ds(i * CH, CH)
        x_copy(i).wait()
        xf = x[rows, :].astype(F32)
        mean = jnp.mean(xf, axis=-1, keepdims=True)
        cen = xf - mean
        rstd = lax.rsqrt(jnp.mean(cen * cen, axis=-1, keepdims=True) + LN_EPS)
        mean_s[rows, :] = mean
        rstd_s[rows, :] = rstd
        u[rows, :] = (cen * rstd * gamma[...] + beta[...]).astype(BF16)

    def qk_chunk(i):
        cols = pl.ds(i * CH, CH)
        res = mm(wt[0:2 * D, :], u[cols, :], NT).astype(BF16)
        for s in range(4):
            qkvt[s // 2, s % 2, :, cols] = res[s * GW:(s + 1) * GW]
        sq = jnp.square(res.astype(F32))
        s_acc[...] += sum(sq[:, 128 * t:128 * t + 128] for t in range(CH // 128))

    gamma_copy.wait()
    beta_copy.wait()
    layer_norm(0)
    w_copy.wait()
    wt[...] = w[...].T
    for i in range(NCH):
        if i + 1 < NCH:
            layer_norm(i + 1)
        qk_chunk(i)

    def compact(full):
        out = jnp.zeros((HD, GW), F32)
        for h in range(4):
            out = jnp.where(heads[h][:, :GW], full[HD * h:HD * h + HD], out)
        return out

    s_col = jnp.sum(s_acc[...], axis=-1, keepdims=True)
    for g in range(2):
        pk1[g, :, 0:GW] = compact(mm(qkvt[0, g], qkvt[1, g], NT))
        blk = pk1[g]
        for h in range(4):
            r = g * GW + h * HD
            blk = jnp.where(lane == GW + h, s_col[r:r + HD], blk)
            blk = jnp.where(lane == GW + 4 + h, s_col[D + r:D + r + HD], blk)
        pk1[g] = blk

    pl.semaphore_wait(barrier, 2)
    a1 = send(0, pk1.at[peer], ra.at[0], partner)

    v_all = mm(wt[2 * D:3 * D, :], u[...], NT).astype(BF16)
    qkvt[2, 0] = v_all[:GW]
    qkvt[2, 1] = v_all[GW:]

    a1.wait_recv()
    sb[0] = pk1[core] + ra[0]
    b1 = send(1, sb.at[0], rb.at[0], other)

    wo_copy.wait()
    dy_copy.wait()
    temp_copy.wait()

    do_all = mm(wo[...], dy[...], NT).astype(BF16)
    dot_[0] = do_all[:GW]
    dot_[1] = do_all[GW:]

    for g in range(2):
        pk2[g, :, 0:GW] = compact(mm(dot_[g], qkvt[2, g], NT))
    a2 = send(2, pk2.at[peer], ra.at[1], partner)

    ut[:, 0:N // 2] = u[0:N // 2, :].T

    a2.wait_recv()
    sb[1] = pk2[core] + ra[1]
    b2 = send(3, sb.at[1], rb.at[1], other)

    ut[:, N // 2:N] = u[N // 2:N, :].T

    def seg_sum(v):
        out = jnp.zeros_like(v)
        for h in range(4):
            out = jnp.where(heads[h], jnp.sum(jnp.where(heads[h], v, 0.0), axis=-1, keepdims=True), out)
        return out

    def expand(dst, g, comp):
        for h in range(4):
            dst[g, HD * h:HD * h + HD, :] = jnp.where(heads[h], comp, 0.0)[:, :GW].astype(BF16)

    b1.wait_recv()
    gs = sb[0] + rb[0]
    rq2 = jnp.zeros((HD, PW), F32)
    rk2 = jnp.zeros((HD, PW), F32)
    tau = jnp.zeros((HD, PW), F32)
    for h in range(4):
        sq_h = jnp.sum(jnp.where(lane == GW + h, gs, 0.0), axis=-1, keepdims=True)
        sk_h = jnp.sum(jnp.where(lane == GW + 4 + h, gs, 0.0), axis=-1, keepdims=True)
        rq2 = jnp.where(heads[h], sq_h, rq2)
        rk2 = jnp.where(eyes[h], sk_h, rk2)
        tau = jnp.where(heads[h], temp[core * 4 + h], tau)
    sk2 = jnp.sum(rk2, axis=0, keepdims=True)
    q_inv = lax.rsqrt(jnp.where(valid, rq2, 1.0))
    k_inv = lax.rsqrt(jnp.where(valid, sk2, 1.0))
    gram = jnp.where(valid, gs, 0.0)
    scores = tau * gram * q_inv * k_inv
    top = jnp.zeros((HD, PW), F32)
    for h in range(4):
        top = jnp.where(heads[h], jnp.max(jnp.where(heads[h], scores, -jnp.inf), axis=-1, keepdims=True), top)
    e = jnp.where(valid, jnp.exp(scores - top), 0.0)
    prob = jnp.where(valid, e / jnp.where(valid, seg_sum(e), 1.0), 0.0)
    cs[0] = prob
    c1 = send(4, cs.at[0], rc.at[0], partner)
    keep[0] = prob
    keep[1] = scores
    keep[2] = gram * q_inv * k_inv
    keep[3] = tau * q_inv * k_inv
    keep[4] = jnp.where(valid, rq2, 1.0)
    keep[5] = jnp.where(valid, jnp.broadcast_to(sk2, (HD, PW)), 1.0)
    expand(abd, core, prob)

    def attend(g):
        ot[g] = mm(abd[g], qkvt[2, g], NN).astype(BF16)

    def d_value(g):
        dqkvt[2, g] = mm(abd[g], dot_[g], TN).astype(BF16)

    attend(core)
    d_value(core)
    c1.wait_recv()
    expand(abd, peer, rc[0])
    attend(peer)

    def all_rows(ref):
        return ref[...].reshape(D, N)

    def weight_send(t):
        return (send(6 + 3 * t, part.at[t, cross], rd1.at[t], partner),
                send(7 + 3 * t, part.at[t, partner], rd2.at[t], partner))

    def link_send(t, first):
        first.wait_recv()
        ls[t] = part[t, other] + rd1[t]
        return send(8 + 3 * t, ls.at[t], rl.at[t], other)

    part[0] = mm(all_rows(ot), dy[...], NN).reshape(4, RB, D)
    d0 = weight_send(0)

    b2.wait_recv()
    da = jnp.where(valid, (sb[1] + rb[1]).astype(BF16).astype(F32), 0.0)
    p = keep[0]
    ds = p * (da - seg_sum(da * p))
    weighted = ds * keep[1]
    dtemp = seg_sum(ds * keep[2])
    dtemp = jnp.sum(dtemp, axis=0, keepdims=True)
    dgram = (ds * keep[3]).astype(BF16).astype(F32)
    dsq = -seg_sum(weighted) / keep[4]
    dsk = -jnp.sum(weighted, axis=0, keepdims=True) / keep[5]
    blk = dgram
    for h in range(4):
        dsk_h = jnp.sum(jnp.where(eyes[h], dsk, 0.0), axis=-1, keepdims=True)
        dsq_h = jnp.sum(jnp.where(eyes[h], dsq, 0.0), axis=-1, keepdims=True)
        dt_h = jnp.sum(jnp.where(lane == HD * h, dtemp, 0.0), axis=-1, keepdims=True)
        blk = jnp.where(lane == GW + h, dsq_h, blk)
        blk = jnp.where(lane == GW + 4 + h, dsk_h, blk)
        blk = jnp.where(lane == GW + 8 + h, dt_h, blk)
    cs[1] = blk
    c2 = send(5, cs.at[1], rc.at[1], partner)

    l0 = link_send(0, d0[0])

    d_value(peer)
    part[1] = mm(all_rows(ut), dqkvt[2].reshape(D, N), NT).reshape(4, RB, D)
    d1 = weight_send(1)

    def d_qk(g, blk):
        expand(gbd, g, jnp.where(valid, blk, 0.0))
        cols = []
        for b in (GW, GW + 4):
            cols.append(jnp.concatenate(
                [jnp.sum(jnp.where(lane == b + h, blk, 0.0), axis=-1, keepdims=True) for h in range(4)], axis=0))
        dqkvt[0, g] = (mm(gbd[g], qkvt[1, g], NN) + qkvt[0, g].astype(F32) * cols[0]).astype(BF16)
        dqkvt[1, g] = (mm(gbd[g], qkvt[0, g], TN) + qkvt[1, g].astype(F32) * cols[1]).astype(BF16)

    d_qk(core, cs[1])
    c2.wait_recv()
    d_qk(peer, rc[1])
    l1 = link_send(1, d1[0])
    part[2] = mm(ut[...], dqkvt[1].reshape(D, N), NT).reshape(4, RB, D)
    d2 = weight_send(2)
    part[3] = mm(ut[...], dqkvt[0].reshape(D, N), NT).reshape(4, RB, D)
    d3 = weight_send(3)
    l2 = link_send(2, d2[0])
    l3 = link_send(3, d3[0])

    lane8 = lax.broadcasted_iota(jnp.int32, (1, 8), 1)
    dt = jnp.zeros((1, 8), F32)
    for g, src in ((core, cs), (peer, rc)):
        head_row = src[1][0:1, :]
        for h in range(4):
            val = jnp.sum(jnp.where(lane[0:1] == GW + 8 + h, head_row, 0.0), axis=-1, keepdims=True)
            dt = jnp.where(lane8 == g * 4 + h, val, dt)
    dt_out[...] = dt

    ot_all = all_rows(ot)
    x_f32 = x[...].astype(F32)
    y_out[...] = (x_f32 + mm(ot_all, wo[...], TN)).astype(BF16)
    dg_sum = jnp.zeros((1, D), F32)
    db_sum = jnp.zeros((1, D), F32)
    for i in range(NCH):
        rows = pl.ds(i * CH, CH)
        dut = mm(w[...], dqkvt[:, :, :, rows].reshape(3 * D, CH), NN).astype(BF16)
        du = dut.T.astype(F32)
        rstd = rstd_s[rows, :]
        xhat = (x[rows, :].astype(F32) - mean_s[rows, :]) * rstd
        dg_sum += jnp.sum(du * xhat, axis=0, keepdims=True)
        db_sum += jnp.sum(du, axis=0, keepdims=True)
        dh = du * gamma[...]
        m1 = jnp.mean(dh, axis=-1, keepdims=True)
        m2 = jnp.mean(dh * xhat, axis=-1, keepdims=True)
        dx_out[rows, :] = (dy[rows, :].astype(F32) + rstd * (dh - m1 - xhat * m2)).astype(BF16)
    es[0:1, :] = dg_sum
    es[1:2, :] = db_sum

    e1 = send(18, es, er.at[0], partner)
    e1.wait()
    er[1] = es[...] + er[0]
    e2 = send(19, er.at[1], er.at[2], other)

    outs = ((dwo_out, slice(0, D)), (dw_out, slice(2 * D, 3 * D)), (dw_out, slice(D, 2 * D)), (dw_out, slice(0, D)))
    for t, (d, l) in enumerate(((d0, l0), (d1, l1), (d2, l2))):
        d[1].wait_recv()
        l.wait_recv()
        outs[t][0][:, outs[t][1]] = (part[t, sp] + rd2[t] + rl[t]).astype(BF16)
    e2.wait()
    tot = er[1] + er[2]
    dg_out[...] = tot[0:1]
    db_out[...] = tot[1:2]
    d3[1].wait_recv()
    l3.wait_recv()
    outs[3][0][:, outs[3][1]] = (part[3, sp] + rd2[3] + rl[3]).astype(BF16)
    for copy in (a1, a2, b1, b2, c1, c2, *d0, *d1, *d2, *d3, l0, l1, l2, l3):
        copy.wait_send()


def write_out(y, dx, dw, dwo, dg, db, dt, y_o, dx_o, dw_o, dwo_o, dg_o, db_o, dt_o, sem):
    copies = [pltpu.make_async_copy(src, dst, sem.at[i]) for i, (src, dst) in enumerate(
        ((y, y_o), (dx, dx_o), (dw, dw_o), (dwo, dwo_o), (dg.at[0], dg_o), (db.at[0], db_o), (dt.at[0], dt_o)))]
    for copy in copies:
        copy.start()
    for copy in copies:
        copy.wait()


def local_step(x_rows, dy_rows, ln_gamma, ln_beta, w_qkv, w_out, temperature):
    hbm = pl.BlockSpec(memory_space=pltpu.HBM)
    vmem = pl.BlockSpec(memory_space=pltpu.VMEM)
    sds = jax.ShapeDtypeStruct
    outs = pl.pallas_call(
        kernel,
        out_shape=(sds((N, D), BF16), sds((N, D), BF16), sds((RB, 3 * D), BF16), sds((RB, D), BF16),
                   sds((1, D), F32), sds((1, D), F32), sds((1, 8), F32)),
        in_specs=[hbm] * 7,
        out_specs=(vmem,) * 7,
        scratch_shapes=[
            pltpu.VMEM((N, D), BF16),
            pltpu.VMEM((N, D), BF16),
            pltpu.VMEM((D, 3 * D), BF16),
            pltpu.VMEM((D, D), BF16),
            pltpu.VMEM((3 * D, D), BF16),
            pltpu.VMEM((N, D), BF16),
            pltpu.VMEM((D, N), BF16),
            pltpu.VMEM((3, 2, GW, N), BF16),
            pltpu.VMEM((3, 2, GW, N), BF16),
            pltpu.VMEM((2, GW, N), BF16),
            pltpu.VMEM((2, GW, N), BF16),
            pltpu.VMEM((N, 1), F32),
            pltpu.VMEM((N, 1), F32),
            pltpu.VMEM((2 * D, 128), F32),
            pltpu.VMEM((2, HD, PW), F32),
            pltpu.VMEM((2, HD, PW), F32),
            pltpu.VMEM((2, HD, PW), F32),
            pltpu.VMEM((2, HD, PW), F32),
            pltpu.VMEM((2, HD, PW), F32),
            pltpu.VMEM((2, HD, PW), F32),
            pltpu.VMEM((2, HD, PW), F32),
            pltpu.VMEM((2, GW, GW), BF16),
            pltpu.VMEM((2, GW, GW), BF16),
            pltpu.VMEM((6, HD, PW), F32),
            pltpu.VMEM((4, 4, RB, D), F32),
            pltpu.VMEM((4, RB, D), F32),
            pltpu.VMEM((4, RB, D), F32),
            pltpu.VMEM((4, RB, D), F32),
            pltpu.VMEM((4, RB, D), F32),
            pltpu.VMEM((8, D), F32),
            pltpu.VMEM((3, 8, D), F32),
            pltpu.VMEM((1, D), F32),
            pltpu.VMEM((1, D), F32),
            pltpu.SMEM((8,), F32),
            pltpu.SemaphoreType.DMA((6,)),
            pltpu.SemaphoreType.DMA((NCH,)),
            pltpu.SemaphoreType.DMA((20,)),
            pltpu.SemaphoreType.DMA((20,)),
        ],
        compiler_params=pltpu.CompilerParams(collective_id=0, has_side_effects=True, vmem_limit_bytes=48 << 20),
        name="xca",
    )(*(pltpu.with_memory_space_constraint(a, pltpu.HBM)
        for a in (x_rows, dy_rows, ln_gamma, ln_beta, w_qkv, w_out, temperature)))
    return pl.pallas_call(
        write_out,
        out_shape=(sds((N, D), BF16), sds((N, D), BF16), sds((RB, 3 * D), BF16), sds((RB, D), BF16),
                   sds((D,), F32), sds((D,), F32), sds((8,), F32)),
        in_specs=[pl.BlockSpec(memory_space=pl.ANY)] * 7,
        out_specs=(hbm,) * 7,
        scratch_shapes=[pltpu.SemaphoreType.DMA((7,))],
        compiler_params=pltpu.CompilerParams(vmem_limit_bytes=1 << 20),
        name="write_out",
    )(*outs)


def solution(mesh):
    row_spec = P(('dp', 'sp'), None)
    full_mat = P(None, None)
    full_vec = P(None)
    part_vec = P('dp')
    return jax.shard_map(local_step, mesh=mesh,
                         in_specs=(row_spec, row_spec, full_vec, full_vec, full_mat, full_mat, full_vec),
                         out_specs=(row_spec, row_spec, row_spec, row_spec, part_vec, part_vec, part_vec),
                         check_vma=False)
```

```python
import jax
import jax.numpy as jnp
from jax import lax
from jax.experimental import pallas as pl
from jax.experimental.pallas import tpu as pltpu
from jax.sharding import PartitionSpec as P

LN_EPS = 1e-6
F32 = jnp.float32
BF16 = jnp.bfloat16
N = 2048
D = 384
HD = 48
GW = 192
PW = 256
RB = 96
CH = 512
NCH = N // CH
LEAD = 1

NN = (((1,), (0,)), ((), ()))
NT = (((1,), (1,)), ((), ()))
TN = (((0,), (0,)), ((), ()))


def mm(a, b, dims):
    return lax.dot_general(a, b, dims, preferred_element_type=F32)


def kernel(x_hbm, dy_hbm, gamma_hbm, beta_hbm, w_hbm, wo_hbm, temp_hbm,
           y_out, dx_out, dw_out, dwo_out, dg_out, db_out, dt_out,
           x, dy, w, wo, wt, u, ut, qkvt, dqkvt, dot_, ot, mean_s, rstd_s, s_acc,
           pk, ra, sb, rb, cs, rc, abd, gbd, keep, part, rd1, rd2, ls, rl, es, er,
           gamma, beta, temp, in_sem, x_sem, ssem, rsem):
    sp = lax.axis_index("sp")
    core = lax.rem(sp, 2)
    oc = 1 - lax.div(sp, 2)
    partner = sp + 1 - 2 * core
    other = lax.rem(sp + 2, 4)
    cross = lax.rem(partner + 2, 4)

    barrier = pltpu.get_barrier_semaphore()
    for dev in (partner, other):
        pl.semaphore_signal(barrier, inc=1, device_id={"sp": dev}, device_id_type=pl.DeviceIdType.MESH)

    qk_cols, v_cols = pl.ds(0, 2 * D), pl.ds(2 * D, D)
    w_copy = pltpu.make_async_copy(w_hbm.at[:, qk_cols], w.at[:, qk_cols], in_sem.at[0])
    wv_copy = pltpu.make_async_copy(w_hbm.at[:, v_cols], w.at[:, v_cols], in_sem.at[6])
    wo_copy = pltpu.make_async_copy(wo_hbm, wo, in_sem.at[1])
    dy_copy = pltpu.make_async_copy(dy_hbm, dy, in_sem.at[2])
    gamma_copy = pltpu.make_async_copy(gamma_hbm, gamma.at[0], in_sem.at[3])
    beta_copy = pltpu.make_async_copy(beta_hbm, beta.at[0], in_sem.at[4])
    temp_copy = pltpu.make_async_copy(temp_hbm, temp, in_sem.at[5])

    def x_copy(i):
        rows = pl.ds(i * CH, CH)
        return pltpu.make_async_copy(x_hbm.at[rows], x.at[rows], x_sem.at[i])

    w_copy.start()
    x_copy(0).start()
    gamma_copy.start()
    beta_copy.start()
    for i in range(1, NCH):
        x_copy(i).start()
    wv_copy.start()
    wo_copy.start()
    dy_copy.start()
    temp_copy.start()

    def remote(slot, src, dst, dev):
        return pltpu.make_async_remote_copy(
            src_ref=src, dst_ref=dst, send_sem=ssem.at[slot], recv_sem=rsem.at[slot],
            device_id={"sp": dev}, device_id_type=pl.DeviceIdType.MESH)

    def send(slot, src, dst, dev):
        copy = remote(slot, src, dst, dev)
        copy.start()
        return copy

    def on_lead(f):
        pl.when(core == LEAD)(f)

    def on_second(f):
        pl.when(core != LEAD)(f)

    a = [remote(p, pk.at[p], ra.at[p], partner) for p in range(2)]
    b = [remote(2 + p, sb.at[p], rb.at[p], other) for p in range(2)]
    c = [remote(4 + p, cs.at[p], rc.at[p], partner) for p in range(2)]

    def lead_sum(p):
        @on_lead
        def _():
            a[p].wait_recv()
            sb[p] = pk[p] + ra[p]
            b[p].start()

    lane = lax.broadcasted_iota(jnp.int32, (HD, PW), 1)
    row = lax.broadcasted_iota(jnp.int32, (HD, PW), 0)
    heads = [(lane >= HD * h) & (lane < HD * h + HD) for h in range(4)]
    eyes = [lane == row + HD * h for h in range(4)]
    valid = lane < GW
    s_acc[...] = jnp.zeros_like(s_acc)
    pk[...] = jnp.zeros_like(pk)
    es[...] = jnp.zeros_like(es)

    def layer_norm(i):
        rows = pl.ds(i * CH, CH)
        x_copy(i).wait()
        xf = x[rows, :].astype(F32)
        mean = jnp.mean(xf, axis=-1, keepdims=True)
        cen = xf - mean
        rstd = lax.rsqrt(jnp.mean(cen * cen, axis=-1, keepdims=True) + LN_EPS)
        mean_s[rows, :] = mean
        rstd_s[rows, :] = rstd
        u[rows, :] = (cen * rstd * gamma[...] + beta[...]).astype(BF16)

    def qk_chunk(i):
        cols = pl.ds(i * CH, CH)
        res = mm(wt[0:2 * D, :], u[cols, :], NT).astype(BF16)
        for s in range(4):
            qkvt[s // 2, s % 2, :, cols] = res[s * GW:(s + 1) * GW]
        sq = jnp.square(res.astype(F32))
        s_acc[...] += sum(sq[:, 128 * t:128 * t + 128] for t in range(CH // 128))

    w_copy.wait()
    wt[0:2 * D, :] = w[:, 0:2 * D].T
    gamma_copy.wait()
    beta_copy.wait()
    layer_norm(0)
    for i in range(NCH):
        if i + 1 < NCH:
            layer_norm(i + 1)
        qk_chunk(i)

    def compact(full):
        out = jnp.zeros((HD, GW), F32)
        for h in range(4):
            out = jnp.where(heads[h][:, :GW], full[HD * h:HD * h + HD], out)
        return out

    s_col = jnp.sum(s_acc[...], axis=-1, keepdims=True)
    for g in range(2):
        pk[0, g, :, 0:GW] = compact(mm(qkvt[0, g], qkvt[1, g], NT))
        blk = pk[0, g]
        for h in range(4):
            r = g * GW + h * HD
            blk = jnp.where(lane == GW + h, s_col[r:r + HD], blk)
            blk = jnp.where(lane == GW + 4 + h, s_col[D + r:D + r + HD], blk)
        pk[0, g] = blk

    pl.semaphore_wait(barrier, 2)

    @on_second
    def _():
        a[0].start()

    wv_copy.wait()
    wt[2 * D:3 * D, :] = w[:, 2 * D:3 * D].T
    v_all = mm(wt[2 * D:3 * D, :], u[...], NT).astype(BF16)
    qkvt[2, 0] = v_all[:GW]
    qkvt[2, 1] = v_all[GW:]
    lead_sum(0)

    wo_copy.wait()
    dy_copy.wait()
    temp_copy.wait()
    do_all = mm(wo[...], dy[...], NT).astype(BF16)
    dot_[0] = do_all[:GW]
    dot_[1] = do_all[GW:]
    for g in range(2):
        pk[1, g, :, 0:GW] = compact(mm(dot_[g], qkvt[2, g], NT))

    @on_second
    def _():
        a[1].start()

    u_t = u[...].T
    ut[0] = u_t[:GW]
    ut[1] = u_t[GW:]
    lead_sum(1)

    def seg_sum(v):
        out = jnp.zeros_like(v)
        for h in range(4):
            out = jnp.where(heads[h], jnp.sum(jnp.where(heads[h], v, 0.0), axis=-1, keepdims=True), out)
        return out

    def expand(dst, g, comp):
        for h in range(4):
            dst[g, HD * h:HD * h + HD, :] = jnp.where(heads[h], comp, 0.0)[:, :GW].astype(BF16)

    def softmax_fwd(g):
        gs = sb[0, g] + rb[0, g]
        rq2 = jnp.zeros((HD, PW), F32)
        rk2 = jnp.zeros((HD, PW), F32)
        tau = jnp.zeros((HD, PW), F32)
        for h in range(4):
            sq_h = jnp.sum(jnp.where(lane == GW + h, gs, 0.0), axis=-1, keepdims=True)
            sk_h = jnp.sum(jnp.where(lane == GW + 4 + h, gs, 0.0), axis=-1, keepdims=True)
            rq2 = jnp.where(heads[h], sq_h, rq2)
            rk2 = jnp.where(eyes[h], sk_h, rk2)
            tau = jnp.where(heads[h], temp[g * 4 + h], tau)
        sk2 = jnp.sum(rk2, axis=0, keepdims=True)
        q_inv = lax.rsqrt(jnp.where(valid, rq2, 1.0))
        k_inv = lax.rsqrt(jnp.where(valid, sk2, 1.0))
        gram = jnp.where(valid, gs, 0.0)
        scores = tau * gram * q_inv * k_inv
        top = jnp.zeros((HD, PW), F32)
        for h in range(4):
            top = jnp.where(heads[h], jnp.max(jnp.where(heads[h], scores, -jnp.inf), axis=-1, keepdims=True), top)
        e = jnp.where(valid, jnp.exp(scores - top), 0.0)
        prob = jnp.where(valid, e / jnp.where(valid, seg_sum(e), 1.0), 0.0)
        cs[0, g] = prob
        keep[0, g] = scores
        keep[1, g] = gram * q_inv * k_inv
        keep[2, g] = tau * q_inv * k_inv
        keep[3, g] = jnp.where(valid, rq2, 1.0)
        keep[4, g] = jnp.where(valid, jnp.broadcast_to(sk2, (HD, PW)), 1.0)

    def softmax_bwd(g):
        da = jnp.where(valid, (sb[1, g] + rb[1, g]).astype(BF16).astype(F32), 0.0)
        p = cs[0, g]
        ds = p * (da - seg_sum(da * p))
        weighted = ds * keep[0, g]
        dtemp = jnp.sum(seg_sum(ds * keep[1, g]), axis=0, keepdims=True)
        dsq = -seg_sum(weighted) / keep[3, g]
        dsk = -jnp.sum(weighted, axis=0, keepdims=True) / keep[4, g]
        blk = (ds * keep[2, g]).astype(BF16).astype(F32)
        for h in range(4):
            dsk_h = jnp.sum(jnp.where(eyes[h], dsk, 0.0), axis=-1, keepdims=True)
            dsq_h = jnp.sum(jnp.where(eyes[h], dsq, 0.0), axis=-1, keepdims=True)
            dt_h = jnp.sum(jnp.where(lane == HD * h, dtemp, 0.0), axis=-1, keepdims=True)
            blk = jnp.where(lane == GW + h, dsq_h, blk)
            blk = jnp.where(lane == GW + 4 + h, dsk_h, blk)
            blk = jnp.where(lane == GW + 8 + h, dt_h, blk)
        cs[1, g] = blk

    @on_lead
    def _():
        b[0].wait_recv()
        for g in range(2):
            softmax_fwd(g)
        c[0].start()
        for g in range(2):
            expand(abd, g, cs[0, g])

    @on_second
    def _():
        c[0].wait_recv()
        for g in range(2):
            expand(abd, g, rc[0, g])

    def attend(g):
        ot[g] = mm(abd[g], qkvt[2, g], NN).astype(BF16)

    def first_send(t):
        return send(6 + 3 * t, part.at[t, cross], rd1.at[t], partner)

    def own_send(t):
        return send(7 + 3 * t, part.at[t, partner], rd2.at[t], partner)

    def link_copy(t):
        return remote(8 + 3 * t, ls.at[t], rl.at[t], other)

    def link_send(t):
        d1[t].wait_recv()
        ls[t] = part[t, other] + rd1[t]
        link_copy(t).start()

    d1, d2 = [None] * 4, [None] * 4
    there, here = pl.ds(2 * oc, 2), pl.ds(2 - 2 * oc, 2)

    attend(oc)
    part[0, there] = mm(ot[oc], dy[...], NN).reshape(2, RB, D)
    d1[0] = first_send(0)

    @on_second
    def _():
        link_send(0)

    for g in range(2):
        dqkvt[2, g] = mm(abd[g], dot_[g], TN).astype(BF16)

    @on_lead
    def _():
        link_send(0)

    part[1, there] = mm(ut[oc], dqkvt[2].reshape(D, N), NT).reshape(2, RB, D)
    d1[1] = first_send(1)

    @on_lead
    def _():
        b[1].wait_recv()
        for g in range(2):
            softmax_bwd(g)
        c[1].start()
        rc[1] = cs[1]

    attend(1 - oc)
    part[0, here] = mm(ot[1 - oc], dy[...], NN).reshape(2, RB, D)
    d2[0] = own_send(0)
    link_send(1)

    @on_second
    def _():
        c[1].wait_recv()

    for g in range(2):
        blk = rc[1, g]
        expand(gbd, g, jnp.where(valid, blk, 0.0))
        cols = []
        for base in (GW, GW + 4):
            cols.append(jnp.concatenate(
                [jnp.sum(jnp.where(lane == base + h, blk, 0.0), axis=-1, keepdims=True) for h in range(4)], axis=0))
        dqkvt[0, g] = (mm(gbd[g], qkvt[1, g], NN) + qkvt[0, g].astype(F32) * cols[0]).astype(BF16)
        dqkvt[1, g] = (mm(gbd[g], qkvt[0, g], TN) + qkvt[1, g].astype(F32) * cols[1]).astype(BF16)

    res = mm(ut[oc], dqkvt[0:2].reshape(2 * D, N), NT)
    part[3, there] = res[:, :D].reshape(2, RB, D)
    part[2, there] = res[:, D:].reshape(2, RB, D)
    d1[2] = first_send(2)
    d1[3] = first_send(3)

    res = mm(ut[1 - oc], dqkvt[...].reshape(3 * D, N), NT)
    for t in (1, 2, 3):
        part[t, here] = res[:, D * (3 - t):D * (4 - t)].reshape(2, RB, D)
        d2[t] = own_send(t)
    link_send(2)
    link_send(3)

    lane8 = lax.broadcasted_iota(jnp.int32, (1, 8), 1)
    dt = jnp.zeros((1, 8), F32)
    for g in range(2):
        head_row = rc[1, g, 0:1, :]
        for h in range(4):
            val = jnp.sum(jnp.where(lane[0:1] == GW + 8 + h, head_row, 0.0), axis=-1, keepdims=True)
            dt = jnp.where(lane8 == g * 4 + h, val, dt)
    dt_out[...] = dt

    dg_sum = jnp.zeros((1, D), F32)
    db_sum = jnp.zeros((1, D), F32)
    for i in range(NCH):
        rows = pl.ds(i * CH, CH)
        dut = mm(w[...], dqkvt[:, :, :, rows].reshape(3 * D, CH), NN).astype(BF16)
        du = dut.T.astype(F32)
        rstd = rstd_s[rows, :]
        xhat = (x[rows, :].astype(F32) - mean_s[rows, :]) * rstd
        dg_sum += jnp.sum(du * xhat, axis=0, keepdims=True)
        db_sum += jnp.sum(du, axis=0, keepdims=True)
        dh = du * gamma[...]
        m1 = jnp.mean(dh, axis=-1, keepdims=True)
        m2 = jnp.mean(dh * xhat, axis=-1, keepdims=True)
        dx_out[rows, :] = (dy[rows, :].astype(F32) + rstd * (dh - m1 - xhat * m2)).astype(BF16)
    es[0:1, :] = dg_sum
    es[1:2, :] = db_sum
    e1 = send(18, es, er.at[0], partner)
    y_out[...] = (x[...].astype(F32) + mm(ot[...].reshape(D, N), wo[...], TN)).astype(BF16)
    e1.wait()
    er[1] = es[...] + er[0]
    e2 = send(19, er.at[1], er.at[2], other)

    outs = ((dwo_out, slice(0, D)), (dw_out, slice(2 * D, 3 * D)), (dw_out, slice(D, 2 * D)), (dw_out, slice(0, D)))
    for t in range(4):
        if t == 3:
            e2.wait()
            tot = er[1] + er[2]
            dg_out[...] = tot[0:1]
            db_out[...] = tot[1:2]
        d2[t].wait_recv()
        link_copy(t).wait_recv()
        outs[t][0][:, outs[t][1]] = (part[t, sp] + rd2[t] + rl[t]).astype(BF16)
    for t in range(4):
        for copy in (d1[t], d2[t], link_copy(t)):
            copy.wait_send()

    @on_lead
    def _():
        for p in range(2):
            b[p].wait_send()
            c[p].wait_send()

    @on_second
    def _():
        for p in range(2):
            a[p].wait_send()


def write_out(y, dx, dw, dwo, dg, db, dt, y_o, dx_o, dw_o, dwo_o, dg_o, db_o, dt_o, sem):
    copies = [pltpu.make_async_copy(src, dst, sem.at[i]) for i, (src, dst) in enumerate(
        ((y, y_o), (dx, dx_o), (dw, dw_o), (dwo, dwo_o), (dg.at[0], dg_o), (db.at[0], db_o), (dt.at[0], dt_o)))]
    for copy in copies:
        copy.start()
    for copy in copies:
        copy.wait()


def local_step(x_rows, dy_rows, ln_gamma, ln_beta, w_qkv, w_out, temperature):
    hbm = pl.BlockSpec(memory_space=pltpu.HBM)
    vmem = pl.BlockSpec(memory_space=pltpu.VMEM)
    sds = jax.ShapeDtypeStruct
    outs = pl.pallas_call(
        kernel,
        out_shape=(sds((N, D), BF16), sds((N, D), BF16), sds((RB, 3 * D), BF16), sds((RB, D), BF16),
                   sds((1, D), F32), sds((1, D), F32), sds((1, 8), F32)),
        in_specs=[hbm] * 7,
        out_specs=(vmem,) * 7,
        scratch_shapes=[
            pltpu.VMEM((N, D), BF16),
            pltpu.VMEM((N, D), BF16),
            pltpu.VMEM((D, 3 * D), BF16),
            pltpu.VMEM((D, D), BF16),
            pltpu.VMEM((3 * D, D), BF16),
            pltpu.VMEM((N, D), BF16),
            pltpu.VMEM((2, GW, N), BF16),
            pltpu.VMEM((3, 2, GW, N), BF16),
            pltpu.VMEM((3, 2, GW, N), BF16),
            pltpu.VMEM((2, GW, N), BF16),
            pltpu.VMEM((2, GW, N), BF16),
            pltpu.VMEM((N, 1), F32),
            pltpu.VMEM((N, 1), F32),
            pltpu.VMEM((2 * D, 128), F32),
            pltpu.VMEM((2, 2, HD, PW), F32),
            pltpu.VMEM((2, 2, HD, PW), F32),
            pltpu.VMEM((2, 2, HD, PW), F32),
            pltpu.VMEM((2, 2, HD, PW), F32),
            pltpu.VMEM((2, 2, HD, PW), F32),
            pltpu.VMEM((2, 2, HD, PW), F32),
            pltpu.VMEM((2, GW, GW), BF16),
            pltpu.VMEM((2, GW, GW), BF16),
            pltpu.VMEM((5, 2, HD, PW), F32),
            pltpu.VMEM((4, 4, RB, D), F32),
            pltpu.VMEM((4, RB, D), F32),
            pltpu.VMEM((4, RB, D), F32),
            pltpu.VMEM((4, RB, D), F32),
            pltpu.VMEM((4, RB, D), F32),
            pltpu.VMEM((8, D), F32),
            pltpu.VMEM((3, 8, D), F32),
            pltpu.VMEM((1, D), F32),
            pltpu.VMEM((1, D), F32),
            pltpu.SMEM((8,), F32),
            pltpu.SemaphoreType.DMA((7,)),
            pltpu.SemaphoreType.DMA((NCH,)),
            pltpu.SemaphoreType.DMA((20,)),
            pltpu.SemaphoreType.DMA((20,)),
        ],
        compiler_params=pltpu.CompilerParams(collective_id=0, has_side_effects=True, vmem_limit_bytes=48 << 20),
        name="xca",
    )(*(pltpu.with_memory_space_constraint(a, pltpu.HBM)
        for a in (x_rows, dy_rows, ln_gamma, ln_beta, w_qkv, w_out, temperature)))
    return pl.pallas_call(
        write_out,
        out_shape=(sds((N, D), BF16), sds((N, D), BF16), sds((RB, 3 * D), BF16), sds((RB, D), BF16),
                   sds((D,), F32), sds((D,), F32), sds((8,), F32)),
        in_specs=[pl.BlockSpec(memory_space=pl.ANY)] * 7,
        out_specs=(hbm,) * 7,
        scratch_shapes=[pltpu.SemaphoreType.DMA((7,))],
        compiler_params=pltpu.CompilerParams(vmem_limit_bytes=1 << 20),
        name="write_out",
    )(*outs)


def solution(mesh):
    row_spec = P(('dp', 'sp'), None)
    full_mat = P(None, None)
    full_vec = P(None)
    part_vec = P('dp')
    return jax.shard_map(local_step, mesh=mesh,
                         in_specs=(row_spec, row_spec, full_vec, full_vec, full_mat, full_mat, full_vec),
                         out_specs=(row_spec, row_spec, row_spec, row_spec, part_vec, part_vec, part_vec),
                         check_vma=False)
```

```python
import jax
import jax.numpy as jnp
from jax import lax
from jax.experimental import pallas as pl
from jax.experimental.pallas import tpu as pltpu
from jax.sharding import PartitionSpec as P

LN_EPS = 1e-6
F32 = jnp.float32
BF16 = jnp.bfloat16
N = 2048
D = 384
HD = 48
GW = 192
PW = 256
RB = 96
CH = 512
NCH = N // CH
LEAD = 0

NN = (((1,), (0,)), ((), ()))
NT = (((1,), (1,)), ((), ()))
TN = (((0,), (0,)), ((), ()))


def mm(a, b, dims):
    return lax.dot_general(a, b, dims, preferred_element_type=F32)


def kernel(x_hbm, dy_hbm, gamma_hbm, beta_hbm, w_hbm, wo_hbm, temp_hbm,
           y_out, dx_out, dw_out, dwo_out, dg_out, db_out, dt_out,
           x, dy, w, wo, wt, u, ut, qkvt, dqkvt, dot_, ot, mean_s, rstd_s, s_acc,
           pk, ra, sb, rb, cs, rc, abd, gbd, keep, part, rd1, rd2, ls, rl, es, er,
           gamma, beta, temp, in_sem, x_sem, ssem, rsem):
    sp = lax.axis_index("sp")
    core = lax.rem(sp, 2)
    oc = 1 - lax.div(sp, 2)
    partner = sp + 1 - 2 * core
    other = lax.rem(sp + 2, 4)
    cross = lax.rem(partner + 2, 4)

    barrier = pltpu.get_barrier_semaphore()
    for dev in (partner, other, cross):
        pl.semaphore_signal(barrier, inc=1, device_id={"sp": dev}, device_id_type=pl.DeviceIdType.MESH)

    qk_cols, v_cols = pl.ds(0, 2 * D), pl.ds(2 * D, D)
    w_copy = pltpu.make_async_copy(w_hbm.at[:, qk_cols], w.at[:, qk_cols], in_sem.at[0])
    wv_copy = pltpu.make_async_copy(w_hbm.at[:, v_cols], w.at[:, v_cols], in_sem.at[6])
    wo_copy = pltpu.make_async_copy(wo_hbm, wo, in_sem.at[1])
    dy_copy = pltpu.make_async_copy(dy_hbm, dy, in_sem.at[2])
    gamma_copy = pltpu.make_async_copy(gamma_hbm, gamma.at[0], in_sem.at[3])
    beta_copy = pltpu.make_async_copy(beta_hbm, beta.at[0], in_sem.at[4])
    temp_copy = pltpu.make_async_copy(temp_hbm, temp, in_sem.at[5])

    def x_copy(i):
        rows = pl.ds(i * CH, CH)
        return pltpu.make_async_copy(x_hbm.at[rows], x.at[rows], x_sem.at[i])

    w_copy.start()
    x_copy(0).start()
    gamma_copy.start()
    beta_copy.start()
    for i in range(1, NCH):
        x_copy(i).start()
    wv_copy.start()
    wo_copy.start()
    dy_copy.start()
    temp_copy.start()

    def remote(slot, src, dst, dev):
        return pltpu.make_async_remote_copy(
            src_ref=src, dst_ref=dst, send_sem=ssem.at[slot], recv_sem=rsem.at[slot],
            device_id={"sp": dev}, device_id_type=pl.DeviceIdType.MESH)

    def send(slot, src, dst, dev):
        copy = remote(slot, src, dst, dev)
        copy.start()
        return copy

    def on_lead(f):
        pl.when(core == LEAD)(f)

    def on_second(f):
        pl.when(core != LEAD)(f)

    a = [remote(p, pk.at[p], ra.at[p], partner) for p in range(2)]
    b = [remote(2 + p, sb.at[p], rb.at[p], other) for p in range(2)]
    c = [remote(4 + p, cs.at[p], rc.at[p], partner) for p in range(2)]

    def lead_sum(p):
        @on_lead
        def _():
            a[p].wait_recv()
            sb[p] = pk[p] + ra[p]
            b[p].start()

    lane = lax.broadcasted_iota(jnp.int32, (HD, PW), 1)
    row = lax.broadcasted_iota(jnp.int32, (HD, PW), 0)
    heads = [(lane >= HD * h) & (lane < HD * h + HD) for h in range(4)]
    eyes = [lane == row + HD * h for h in range(4)]
    valid = lane < GW
    s_acc[...] = jnp.zeros_like(s_acc)
    pk[...] = jnp.zeros_like(pk)

    def layer_norm(i):
        rows = pl.ds(i * CH, CH)
        x_copy(i).wait()
        xf = x[rows, :].astype(F32)
        mean = jnp.mean(xf, axis=-1, keepdims=True)
        cen = xf - mean
        rstd = lax.rsqrt(jnp.mean(cen * cen, axis=-1, keepdims=True) + LN_EPS)
        mean_s[rows, :] = mean
        rstd_s[rows, :] = rstd
        u[rows, :] = (cen * rstd * gamma[...] + beta[...]).astype(BF16)

    def qk_chunk(i):
        cols = pl.ds(i * CH, CH)
        res = mm(wt[0:2 * D, :], u[cols, :], NT).astype(BF16)
        for s in range(4):
            qkvt[s // 2, s % 2, :, cols] = res[s * GW:(s + 1) * GW]
        sq = jnp.square(res.astype(F32))
        s_acc[...] += sum(sq[:, 128 * t:128 * t + 128] for t in range(CH // 128))

    w_copy.wait()
    wt[0:2 * D, :] = w[:, 0:2 * D].T
    gamma_copy.wait()
    beta_copy.wait()
    layer_norm(0)
    for i in range(NCH):
        if i + 1 < NCH:
            layer_norm(i + 1)
        qk_chunk(i)

    def compact(full):
        out = jnp.zeros((HD, GW), F32)
        for h in range(4):
            out = jnp.where(heads[h][:, :GW], full[HD * h:HD * h + HD], out)
        return out

    s_col = jnp.sum(s_acc[...], axis=-1, keepdims=True)
    for g in range(2):
        pk[0, g, :, 0:GW] = compact(mm(qkvt[0, g], qkvt[1, g], NT))
        blk = pk[0, g]
        for h in range(4):
            r = g * GW + h * HD
            blk = jnp.where(lane == GW + h, s_col[r:r + HD], blk)
            blk = jnp.where(lane == GW + 4 + h, s_col[D + r:D + r + HD], blk)
        pk[0, g] = blk

    pl.semaphore_wait(barrier, 3)

    @on_second
    def _():
        a[0].start()

    wv_copy.wait()
    wt[2 * D:3 * D, :] = w[:, 2 * D:3 * D].T
    u_t = u[...].T
    ut[0] = u_t[:GW]
    ut[1] = u_t[GW:]
    lead_sum(0)
    v_all = mm(wt[2 * D:3 * D, :], u[...], NT).astype(BF16)
    qkvt[2, 0] = v_all[:GW]
    qkvt[2, 1] = v_all[GW:]

    wo_copy.wait()
    dy_copy.wait()
    temp_copy.wait()
    do_all = mm(wo[...], dy[...], NT).astype(BF16)
    dot_[0] = do_all[:GW]
    dot_[1] = do_all[GW:]
    for g in range(2):
        pk[1, g, :, 0:GW] = compact(mm(dot_[g], qkvt[2, g], NT))

    @on_second
    def _():
        a[1].start()

    lead_sum(1)

    def seg_sum(v):
        out = jnp.zeros_like(v)
        for h in range(4):
            out = jnp.where(heads[h], jnp.sum(jnp.where(heads[h], v, 0.0), axis=-1, keepdims=True), out)
        return out

    def expand(dst, g, comp):
        for h in range(4):
            dst[g, HD * h:HD * h + HD, :] = jnp.where(heads[h], comp, 0.0)[:, :GW].astype(BF16)

    def softmax_fwd(g):
        gs = sb[0, g] + rb[0, g]
        rq2 = jnp.zeros((HD, PW), F32)
        rk2 = jnp.zeros((HD, PW), F32)
        tau = jnp.zeros((HD, PW), F32)
        for h in range(4):
            sq_h = jnp.sum(jnp.where(lane == GW + h, gs, 0.0), axis=-1, keepdims=True)
            sk_h = jnp.sum(jnp.where(lane == GW + 4 + h, gs, 0.0), axis=-1, keepdims=True)
            rq2 = jnp.where(heads[h], sq_h, rq2)
            rk2 = jnp.where(eyes[h], sk_h, rk2)
            tau = jnp.where(heads[h], temp[g * 4 + h], tau)
        sk2 = jnp.sum(rk2, axis=0, keepdims=True)
        q_inv = lax.rsqrt(jnp.where(valid, rq2, 1.0))
        k_inv = lax.rsqrt(jnp.where(valid, sk2, 1.0))
        gram = jnp.where(valid, gs, 0.0)
        scores = tau * gram * q_inv * k_inv
        top = jnp.zeros((HD, PW), F32)
        for h in range(4):
            top = jnp.where(heads[h], jnp.max(jnp.where(heads[h], scores, -jnp.inf), axis=-1, keepdims=True), top)
        e = jnp.where(valid, jnp.exp(scores - top), 0.0)
        prob = jnp.where(valid, e / jnp.where(valid, seg_sum(e), 1.0), 0.0)
        cs[0, g] = prob
        keep[0, g] = scores
        keep[1, g] = gram * q_inv * k_inv
        keep[2, g] = tau * q_inv * k_inv
        keep[3, g] = jnp.where(valid, rq2, 1.0)
        keep[4, g] = jnp.where(valid, jnp.broadcast_to(sk2, (HD, PW)), 1.0)

    def softmax_bwd(g):
        da = jnp.where(valid, (sb[1, g] + rb[1, g]).astype(BF16).astype(F32), 0.0)
        p = cs[0, g]
        ds = p * (da - seg_sum(da * p))
        weighted = ds * keep[0, g]
        dtemp = jnp.sum(seg_sum(ds * keep[1, g]), axis=0, keepdims=True)
        dsq = -seg_sum(weighted) / keep[3, g]
        dsk = -jnp.sum(weighted, axis=0, keepdims=True) / keep[4, g]
        blk = (ds * keep[2, g]).astype(BF16).astype(F32)
        for h in range(4):
            dsk_h = jnp.sum(jnp.where(eyes[h], dsk, 0.0), axis=-1, keepdims=True)
            dsq_h = jnp.sum(jnp.where(eyes[h], dsq, 0.0), axis=-1, keepdims=True)
            dt_h = jnp.sum(jnp.where(lane == HD * h, dtemp, 0.0), axis=-1, keepdims=True)
            blk = jnp.where(lane == GW + h, dsq_h, blk)
            blk = jnp.where(lane == GW + 4 + h, dsk_h, blk)
            blk = jnp.where(lane == GW + 8 + h, dt_h, blk)
        cs[1, g] = blk

    @on_lead
    def _():
        b[0].wait_recv()
        for g in range(2):
            softmax_fwd(g)
        c[0].start()
        for g in range(2):
            expand(abd, g, cs[0, g])

    @on_second
    def _():
        c[0].wait_recv()
        for g in range(2):
            expand(abd, g, rc[0, g])

    def attend(g):
        ot[g] = mm(abd[g], qkvt[2, g], NN).astype(BF16)

    def first_send(t):
        return send(6 + 3 * t, part.at[t, cross], rd1.at[t], partner)

    def own_send(t):
        return send(7 + 3 * t, part.at[t, partner], rd2.at[t], partner)

    def link_copy(t):
        return remote(8 + 3 * t, ls.at[t], rl.at[t], other)

    def link_send(t):
        d1[t].wait_recv()
        ls[t] = part[t, other] + rd1[t]
        link_copy(t).start()

    d1, d2 = [None] * 4, [None] * 4
    there, here = pl.ds(2 * oc, 2), pl.ds(2 - 2 * oc, 2)

    attend(oc)
    part[0, there] = mm(ot[oc], dy[...], NN).reshape(2, RB, D)
    d1[0] = first_send(0)

    @on_second
    def _():
        link_send(0)

    for g in range(2):
        dqkvt[2, g] = mm(abd[g], dot_[g], TN).astype(BF16)

    part[1, there] = mm(ut[oc], dqkvt[2].reshape(D, N), NT).reshape(2, RB, D)
    d1[1] = first_send(1)

    @on_second
    def _():
        link_send(1)

    @on_lead
    def _():
        b[1].wait_recv()
        for g in range(2):
            softmax_bwd(g)
        c[1].start()
        rc[1] = cs[1]

    attend(1 - oc)
    part[0, here] = mm(ot[1 - oc], dy[...], NN).reshape(2, RB, D)
    d2[0] = own_send(0)

    @on_lead
    def _():
        link_send(0)

    @on_second
    def _():
        c[1].wait_recv()

    for g in range(2):
        blk = rc[1, g]
        expand(gbd, g, jnp.where(valid, blk, 0.0))
        cols = []
        for base in (GW, GW + 4):
            cols.append(jnp.concatenate(
                [jnp.sum(jnp.where(lane == base + h, blk, 0.0), axis=-1, keepdims=True) for h in range(4)], axis=0))
        dqkvt[0, g] = (mm(gbd[g], qkvt[1, g], NN) + qkvt[0, g].astype(F32) * cols[0]).astype(BF16)
        dqkvt[1, g] = (mm(gbd[g], qkvt[0, g], TN) + qkvt[1, g].astype(F32) * cols[1]).astype(BF16)

    @on_lead
    def _():
        link_send(1)

    res = mm(ut[oc], dqkvt[0:2].reshape(2 * D, N), NT)
    part[3, there] = res[:, :D].reshape(2, RB, D)
    part[2, there] = res[:, D:].reshape(2, RB, D)
    d1[2] = first_send(2)
    d1[3] = first_send(3)

    lane8 = lax.broadcasted_iota(jnp.int32, (1, 8), 1)
    dt = jnp.zeros((1, 8), F32)
    for g in range(2):
        head_row = rc[1, g, 0:1, :]
        for h in range(4):
            val = jnp.sum(jnp.where(lane[0:1] == GW + 8 + h, head_row, 0.0), axis=-1, keepdims=True)
            dt = jnp.where(lane8 == g * 4 + h, val, dt)
    dt_out[...] = dt

    dg_sum = jnp.zeros((1, D), F32)
    db_sum = jnp.zeros((1, D), F32)
    for i in range(NCH):
        if i == NCH // 2:
            @on_lead
            def _():
                link_send(2)
                link_send(3)

        rows = pl.ds(i * CH, CH)
        dut = mm(w[...], dqkvt[:, :, :, rows].reshape(3 * D, CH), NN).astype(BF16)
        du = dut.T.astype(F32)
        rstd = rstd_s[rows, :]
        xhat = (x[rows, :].astype(F32) - mean_s[rows, :]) * rstd
        dg_sum += jnp.sum(du * xhat, axis=0, keepdims=True)
        db_sum += jnp.sum(du, axis=0, keepdims=True)
        dh = du * gamma[...]
        m1 = jnp.mean(dh, axis=-1, keepdims=True)
        m2 = jnp.mean(dh * xhat, axis=-1, keepdims=True)
        dx_out[rows, :] = (dy[rows, :].astype(F32) + rstd * (dh - m1 - xhat * m2)).astype(BF16)
    es[0:1, :] = dg_sum
    es[1:2, :] = db_sum
    ecopies = [send(18 + i, es, er.at[i], dev) for i, dev in enumerate((partner, other, cross))]

    @on_second
    def _():
        link_send(2)
        link_send(3)

    res = mm(ut[1 - oc], dqkvt[...].reshape(3 * D, N), NT)
    for t in (1, 2, 3):
        part[t, here] = res[:, D * (3 - t):D * (4 - t)].reshape(2, RB, D)
        d2[t] = own_send(t)
    y_out[...] = (x[...].astype(F32) + mm(ot[...].reshape(D, N), wo[...], TN)).astype(BF16)

    outs = ((dwo_out, slice(0, D)), (dw_out, slice(2 * D, 3 * D)), (dw_out, slice(D, 2 * D)), (dw_out, slice(0, D)))
    for t in range(4):
        d2[t].wait_recv()
    for copy in ecopies:
        copy.wait()
    tot = (es[...] + er[0]) + (er[1] + er[2])
    dg_out[...] = tot[0:1]
    db_out[...] = tot[1:2]
    for t in range(4):
        link_copy(t).wait_recv()
        outs[t][0][:, outs[t][1]] = (part[t, sp] + rd2[t] + rl[t]).astype(BF16)
    for t in range(4):
        for copy in (d1[t], d2[t], link_copy(t)):
            copy.wait_send()

    @on_lead
    def _():
        for p in range(2):
            b[p].wait_send()
            c[p].wait_send()

    @on_second
    def _():
        for p in range(2):
            a[p].wait_send()


def write_out(y, dx, dw, dwo, dg, db, dt, y_o, dx_o, dw_o, dwo_o, dg_o, db_o, dt_o, sem):
    copies = [pltpu.make_async_copy(src, dst, sem.at[i]) for i, (src, dst) in enumerate(
        ((y, y_o), (dx, dx_o), (dw, dw_o), (dwo, dwo_o), (dg.at[0], dg_o), (db.at[0], db_o), (dt.at[0], dt_o)))]
    for copy in copies:
        copy.start()
    for copy in copies:
        copy.wait()


def local_step(x_rows, dy_rows, ln_gamma, ln_beta, w_qkv, w_out, temperature):
    hbm = pl.BlockSpec(memory_space=pltpu.HBM)
    vmem = pl.BlockSpec(memory_space=pltpu.VMEM)
    sds = jax.ShapeDtypeStruct
    outs = pl.pallas_call(
        kernel,
        out_shape=(sds((N, D), BF16), sds((N, D), BF16), sds((RB, 3 * D), BF16), sds((RB, D), BF16),
                   sds((1, D), F32), sds((1, D), F32), sds((1, 8), F32)),
        in_specs=[hbm] * 7,
        out_specs=(vmem,) * 7,
        scratch_shapes=[
            pltpu.VMEM((N, D), BF16),
            pltpu.VMEM((N, D), BF16),
            pltpu.VMEM((D, 3 * D), BF16),
            pltpu.VMEM((D, D), BF16),
            pltpu.VMEM((3 * D, D), BF16),
            pltpu.VMEM((N, D), BF16),
            pltpu.VMEM((2, GW, N), BF16),
            pltpu.VMEM((3, 2, GW, N), BF16),
            pltpu.VMEM((3, 2, GW, N), BF16),
            pltpu.VMEM((2, GW, N), BF16),
            pltpu.VMEM((2, GW, N), BF16),
            pltpu.VMEM((N, 1), F32),
            pltpu.VMEM((N, 1), F32),
            pltpu.VMEM((2 * D, 128), F32),
            pltpu.VMEM((2, 2, HD, PW), F32),
            pltpu.VMEM((2, 2, HD, PW), F32),
            pltpu.VMEM((2, 2, HD, PW), F32),
            pltpu.VMEM((2, 2, HD, PW), F32),
            pltpu.VMEM((2, 2, HD, PW), F32),
            pltpu.VMEM((2, 2, HD, PW), F32),
            pltpu.VMEM((2, GW, GW), BF16),
            pltpu.VMEM((2, GW, GW), BF16),
            pltpu.VMEM((5, 2, HD, PW), F32),
            pltpu.VMEM((4, 4, RB, D), F32),
            pltpu.VMEM((4, RB, D), F32),
            pltpu.VMEM((4, RB, D), F32),
            pltpu.VMEM((4, RB, D), F32),
            pltpu.VMEM((4, RB, D), F32),
            pltpu.VMEM((2, D), F32),
            pltpu.VMEM((3, 2, D), F32),
            pltpu.VMEM((1, D), F32),
            pltpu.VMEM((1, D), F32),
            pltpu.SMEM((8,), F32),
            pltpu.SemaphoreType.DMA((7,)),
            pltpu.SemaphoreType.DMA((NCH,)),
            pltpu.SemaphoreType.DMA((21,)),
            pltpu.SemaphoreType.DMA((21,)),
        ],
        compiler_params=pltpu.CompilerParams(collective_id=0, has_side_effects=True, vmem_limit_bytes=48 << 20),
        name="xca",
    )(*(pltpu.with_memory_space_constraint(a, pltpu.HBM)
        for a in (x_rows, dy_rows, ln_gamma, ln_beta, w_qkv, w_out, temperature)))
    return pl.pallas_call(
        write_out,
        out_shape=(sds((N, D), BF16), sds((N, D), BF16), sds((RB, 3 * D), BF16), sds((RB, D), BF16),
                   sds((D,), F32), sds((D,), F32), sds((8,), F32)),
        in_specs=[pl.BlockSpec(memory_space=pl.ANY)] * 7,
        out_specs=(hbm,) * 7,
        scratch_shapes=[pltpu.SemaphoreType.DMA((7,))],
        compiler_params=pltpu.CompilerParams(vmem_limit_bytes=1 << 20),
        name="write_out",
    )(*outs)


def solution(mesh):
    row_spec = P(('dp', 'sp'), None)
    full_mat = P(None, None)
    full_vec = P(None)
    part_vec = P('dp')
    return jax.shard_map(local_step, mesh=mesh,
                         in_specs=(row_spec, row_spec, full_vec, full_vec, full_mat, full_mat, full_vec),
                         out_specs=(row_spec, row_spec, row_spec, row_spec, part_vec, part_vec, part_vec),
                         check_vma=False)
```

```python
import jax
import jax.numpy as jnp
from jax import lax
from jax.experimental import pallas as pl
from jax.experimental.pallas import tpu as pltpu
from jax.sharding import PartitionSpec as P

LN_EPS = 1e-6
F32 = jnp.float32
BF16 = jnp.bfloat16
N = 2048
D = 384
HD = 48
GW = 192
PW = 256
RB = 96
CH = 512
NCH = N // CH
STARTS = (0, 512, 1024)
SIZES = (512, 512, 1024)
LEAD = 0

NN = (((1,), (0,)), ((), ()))
NT = (((1,), (1,)), ((), ()))
TN = (((0,), (0,)), ((), ()))


def mm(a, b, dims):
    return lax.dot_general(a, b, dims, preferred_element_type=F32)


def kernel(x_hbm, dy_hbm, gamma_hbm, beta_hbm, w_hbm, wo_hbm, temp_hbm,
           y_out, dx_out, dw_out, dwo_out, dg_out, db_out, dt_out,
           x, dy, w, wo, wt, u, ut, qkvt, dqkvt, dot_, ot, mean_s, rstd_s, s_acc,
           pk, ra, sb, rb, cs, rc, abd, gbd, keep, part, rd1, rd2, ls, rl, es, er,
           gamma, beta, temp, in_sem, x_sem, ssem, rsem):
    sp = lax.axis_index("sp")
    core = lax.rem(sp, 2)
    oc = 1 - lax.div(sp, 2)
    partner = sp + 1 - 2 * core
    other = lax.rem(sp + 2, 4)
    cross = lax.rem(partner + 2, 4)

    barrier = pltpu.get_barrier_semaphore()
    for dev in (partner, other, cross):
        pl.semaphore_signal(barrier, inc=1, device_id={"sp": dev}, device_id_type=pl.DeviceIdType.MESH)

    qk_cols, v_cols = pl.ds(0, 2 * D), pl.ds(2 * D, D)
    w_copy = pltpu.make_async_copy(w_hbm.at[:, qk_cols], w.at[:, qk_cols], in_sem.at[0])
    wv_copy = pltpu.make_async_copy(w_hbm.at[:, v_cols], w.at[:, v_cols], in_sem.at[6])
    wo_copy = pltpu.make_async_copy(wo_hbm, wo, in_sem.at[1])
    dy_copy = pltpu.make_async_copy(dy_hbm, dy, in_sem.at[2])
    gamma_copy = pltpu.make_async_copy(gamma_hbm, gamma.at[0], in_sem.at[3])
    beta_copy = pltpu.make_async_copy(beta_hbm, beta.at[0], in_sem.at[4])
    temp_copy = pltpu.make_async_copy(temp_hbm, temp, in_sem.at[5])

    def x_copy(i):
        rows = pl.ds(STARTS[i], SIZES[i])
        return pltpu.make_async_copy(x_hbm.at[rows], x.at[rows], x_sem.at[i])

    w_copy.start()
    x_copy(0).start()
    gamma_copy.start()
    beta_copy.start()
    for i in range(1, len(SIZES)):
        x_copy(i).start()
    wv_copy.start()
    wo_copy.start()
    dy_copy.start()
    temp_copy.start()

    def remote(slot, src, dst, dev):
        return pltpu.make_async_remote_copy(
            src_ref=src, dst_ref=dst, send_sem=ssem.at[slot], recv_sem=rsem.at[slot],
            device_id={"sp": dev}, device_id_type=pl.DeviceIdType.MESH)

    def send(slot, src, dst, dev):
        copy = remote(slot, src, dst, dev)
        copy.start()
        return copy

    def on_lead(f):
        pl.when(core == LEAD)(f)

    def on_second(f):
        pl.when(core != LEAD)(f)

    a = [remote(p, pk.at[p], ra.at[p], partner) for p in range(2)]
    b = [remote(2 + p, sb.at[p], rb.at[p], other) for p in range(2)]
    c = [remote(4 + p, cs.at[p], rc.at[p], partner) for p in range(2)]

    def lead_sum(p):
        @on_lead
        def _():
            a[p].wait_recv()
            sb[p] = pk[p] + ra[p]
            b[p].start()

    lane = lax.broadcasted_iota(jnp.int32, (HD, PW), 1)
    row = lax.broadcasted_iota(jnp.int32, (HD, PW), 0)
    heads = [(lane >= HD * h) & (lane < HD * h + HD) for h in range(4)]
    eyes = [lane == row + HD * h for h in range(4)]
    valid = lane < GW
    s_acc[...] = jnp.zeros_like(s_acc)
    pk[...] = jnp.zeros_like(pk)

    def layer_norm(i):
        rows = pl.ds(STARTS[i], SIZES[i])
        x_copy(i).wait()
        xf = x[rows, :].astype(F32)
        mean = jnp.mean(xf, axis=-1, keepdims=True)
        cen = xf - mean
        rstd = lax.rsqrt(jnp.mean(cen * cen, axis=-1, keepdims=True) + LN_EPS)
        mean_s[rows, :] = mean
        rstd_s[rows, :] = rstd
        u[rows, :] = (cen * rstd * gamma[...] + beta[...]).astype(BF16)

    def qk_chunk(i):
        cols = pl.ds(STARTS[i], SIZES[i])
        res = mm(wt[0:2 * D, :], u[cols, :], NT).astype(BF16)
        for s in range(4):
            qkvt[s // 2, s % 2, :, cols] = res[s * GW:(s + 1) * GW]
        sq = jnp.square(res.astype(F32))
        s_acc[...] += sum(sq[:, 128 * t:128 * t + 128] for t in range(SIZES[i] // 128))

    w_copy.wait()
    wt[0:2 * D, :] = w[:, 0:2 * D].T
    gamma_copy.wait()
    beta_copy.wait()
    layer_norm(0)
    for i in range(len(SIZES)):
        if i + 1 < len(SIZES):
            layer_norm(i + 1)
        qk_chunk(i)

    def compact(full):
        out = jnp.zeros((HD, GW), F32)
        for h in range(4):
            out = jnp.where(heads[h][:, :GW], full[HD * h:HD * h + HD], out)
        return out

    s_col = jnp.sum(s_acc[...], axis=-1, keepdims=True)
    for g in range(2):
        pk[0, g, :, 0:GW] = compact(mm(qkvt[0, g], qkvt[1, g], NT))
        blk = pk[0, g]
        for h in range(4):
            r = g * GW + h * HD
            blk = jnp.where(lane == GW + h, s_col[r:r + HD], blk)
            blk = jnp.where(lane == GW + 4 + h, s_col[D + r:D + r + HD], blk)
        pk[0, g] = blk

    pl.semaphore_wait(barrier, 3)

    @on_second
    def _():
        a[0].start()

    wv_copy.wait()
    wt[2 * D:3 * D, :] = w[:, 2 * D:3 * D].T
    u_t = u[...].T
    ut[0] = u_t[:GW]
    ut[1] = u_t[GW:]
    lead_sum(0)
    v_all = mm(wt[2 * D:3 * D, :], u[...], NT).astype(BF16)
    qkvt[2, 0] = v_all[:GW]
    qkvt[2, 1] = v_all[GW:]

    wo_copy.wait()
    dy_copy.wait()
    temp_copy.wait()
    do_all = mm(wo[...], dy[...], NT).astype(BF16)
    dot_[0] = do_all[:GW]
    dot_[1] = do_all[GW:]
    for g in range(2):
        pk[1, g, :, 0:GW] = compact(mm(dot_[g], qkvt[2, g], NT))

    @on_second
    def _():
        a[1].start()

    lead_sum(1)

    def seg_sum(v):
        out = jnp.zeros_like(v)
        for h in range(4):
            out = jnp.where(heads[h], jnp.sum(jnp.where(heads[h], v, 0.0), axis=-1, keepdims=True), out)
        return out

    def expand(dst, g, comp):
        for h in range(4):
            dst[g, HD * h:HD * h + HD, :] = jnp.where(heads[h], comp, 0.0)[:, :GW].astype(BF16)

    def softmax_fwd(g):
        gs = sb[0, g] + rb[0, g]
        rq2 = jnp.zeros((HD, PW), F32)
        rk2 = jnp.zeros((HD, PW), F32)
        tau = jnp.zeros((HD, PW), F32)
        for h in range(4):
            sq_h = jnp.sum(jnp.where(lane == GW + h, gs, 0.0), axis=-1, keepdims=True)
            sk_h = jnp.sum(jnp.where(lane == GW + 4 + h, gs, 0.0), axis=-1, keepdims=True)
            rq2 = jnp.where(heads[h], sq_h, rq2)
            rk2 = jnp.where(eyes[h], sk_h, rk2)
            tau = jnp.where(heads[h], temp[g * 4 + h], tau)
        sk2 = jnp.sum(rk2, axis=0, keepdims=True)
        q_inv = lax.rsqrt(jnp.where(valid, rq2, 1.0))
        k_inv = lax.rsqrt(jnp.where(valid, sk2, 1.0))
        gram = jnp.where(valid, gs, 0.0)
        scores = tau * gram * q_inv * k_inv
        top = jnp.zeros((HD, PW), F32)
        for h in range(4):
            top = jnp.where(heads[h], jnp.max(jnp.where(heads[h], scores, -jnp.inf), axis=-1, keepdims=True), top)
        e = jnp.where(valid, jnp.exp(scores - top), 0.0)
        prob = jnp.where(valid, e / jnp.where(valid, seg_sum(e), 1.0), 0.0)
        cs[0, g] = prob
        keep[0, g] = scores
        keep[1, g] = gram * q_inv * k_inv
        keep[2, g] = tau * q_inv * k_inv
        keep[3, g] = jnp.where(valid, rq2, 1.0)
        keep[4, g] = jnp.where(valid, jnp.broadcast_to(sk2, (HD, PW)), 1.0)

    def softmax_bwd(g):
        da = jnp.where(valid, (sb[1, g] + rb[1, g]).astype(BF16).astype(F32), 0.0)
        p = cs[0, g]
        ds = p * (da - seg_sum(da * p))
        weighted = ds * keep[0, g]
        dtemp = jnp.sum(seg_sum(ds * keep[1, g]), axis=0, keepdims=True)
        dsq = -seg_sum(weighted) / keep[3, g]
        dsk = -jnp.sum(weighted, axis=0, keepdims=True) / keep[4, g]
        blk = (ds * keep[2, g]).astype(BF16).astype(F32)
        for h in range(4):
            dsk_h = jnp.sum(jnp.where(eyes[h], dsk, 0.0), axis=-1, keepdims=True)
            dsq_h = jnp.sum(jnp.where(eyes[h], dsq, 0.0), axis=-1, keepdims=True)
            dt_h = jnp.sum(jnp.where(lane == HD * h, dtemp, 0.0), axis=-1, keepdims=True)
            blk = jnp.where(lane == GW + h, dsq_h, blk)
            blk = jnp.where(lane == GW + 4 + h, dsk_h, blk)
            blk = jnp.where(lane == GW + 8 + h, dt_h, blk)
        cs[1, g] = blk

    @on_lead
    def _():
        b[0].wait_recv()
        for g in range(2):
            softmax_fwd(g)
        c[0].start()
        for g in range(2):
            expand(abd, g, cs[0, g])

    @on_second
    def _():
        c[0].wait_recv()
        for g in range(2):
            expand(abd, g, rc[0, g])

    def attend(g):
        ot[g] = mm(abd[g], qkvt[2, g], NN).astype(BF16)

    def first_send(t):
        return send(6 + 3 * t, part.at[t, cross], rd1.at[t], partner)

    def own_send(t):
        return send(7 + 3 * t, part.at[t, partner], rd2.at[t], partner)

    def link_copy(t):
        return remote(8 + 3 * t, ls.at[t], rl.at[t], other)

    def link_send(t):
        d1[t].wait_recv()
        ls[t] = part[t, other] + rd1[t]
        link_copy(t).start()

    d1, d2 = [None] * 4, [None] * 4
    there, here = pl.ds(2 * oc, 2), pl.ds(2 - 2 * oc, 2)

    attend(oc)
    part[0, there] = mm(ot[oc], dy[...], NN).reshape(2, RB, D)
    d1[0] = first_send(0)

    @on_second
    def _():
        link_send(0)

    for g in range(2):
        dqkvt[2, g] = mm(abd[g], dot_[g], TN).astype(BF16)

    part[1] = mm(ut[...].reshape(D, N), dqkvt[2].reshape(D, N), NT).reshape(4, RB, D)
    d1[1] = first_send(1)
    d2[1] = own_send(1)

    @on_second
    def _():
        link_send(1)

    @on_lead
    def _():
        b[1].wait_recv()
        for g in range(2):
            softmax_bwd(g)
        c[1].start()
        rc[1] = cs[1]

    @on_second
    def _():
        c[1].wait_recv()

    for g in range(2):
        blk = rc[1, g]
        expand(gbd, g, jnp.where(valid, blk, 0.0))
        cols = []
        for base in (GW, GW + 4):
            cols.append(jnp.concatenate(
                [jnp.sum(jnp.where(lane == base + h, blk, 0.0), axis=-1, keepdims=True) for h in range(4)], axis=0))
        dqkvt[0, g] = (mm(gbd[g], qkvt[1, g], NN) + qkvt[0, g].astype(F32) * cols[0]).astype(BF16)
        dqkvt[1, g] = (mm(gbd[g], qkvt[0, g], TN) + qkvt[1, g].astype(F32) * cols[1]).astype(BF16)

    @on_lead
    def _():
        link_send(0)

    res = mm(ut[oc], dqkvt[0:2].reshape(2 * D, N), NT)
    part[3, there] = res[:, :D].reshape(2, RB, D)
    part[2, there] = res[:, D:].reshape(2, RB, D)
    d1[2] = first_send(2)
    d1[3] = first_send(3)

    @on_lead
    def _():
        link_send(1)


    lane8 = lax.broadcasted_iota(jnp.int32, (1, 8), 1)
    dt = jnp.zeros((1, 8), F32)
    for g in range(2):
        head_row = rc[1, g, 0:1, :]
        for h in range(4):
            val = jnp.sum(jnp.where(lane[0:1] == GW + 8 + h, head_row, 0.0), axis=-1, keepdims=True)
            dt = jnp.where(lane8 == g * 4 + h, val, dt)
    dt_out[...] = dt

    dg_sum = jnp.zeros((1, D), F32)
    db_sum = jnp.zeros((1, D), F32)
    for i in range(NCH):
        if i == NCH // 2:
            @on_lead
            def _():
                link_send(2)
                link_send(3)

        rows = pl.ds(i * CH, CH)
        dut = mm(w[...], dqkvt[:, :, :, rows].reshape(3 * D, CH), NN).astype(BF16)
        du = dut.T.astype(F32)
        rstd = rstd_s[rows, :]
        xhat = (x[rows, :].astype(F32) - mean_s[rows, :]) * rstd
        dg_sum += jnp.sum(du * xhat, axis=0, keepdims=True)
        db_sum += jnp.sum(du, axis=0, keepdims=True)
        dh = du * gamma[...]
        m1 = jnp.mean(dh, axis=-1, keepdims=True)
        m2 = jnp.mean(dh * xhat, axis=-1, keepdims=True)
        dx_out[rows, :] = (dy[rows, :].astype(F32) + rstd * (dh - m1 - xhat * m2)).astype(BF16)
    es[0:1, :] = dg_sum
    es[1:2, :] = db_sum
    ecopies = [send(18 + i, es, er.at[i], dev) for i, dev in enumerate((partner, other, cross))]

    @on_second
    def _():
        link_send(2)
        link_send(3)

    attend(1 - oc)
    part[0, here] = mm(ot[1 - oc], dy[...], NN).reshape(2, RB, D)
    d2[0] = own_send(0)
    res = mm(ut[1 - oc], dqkvt[0:2].reshape(2 * D, N), NT)
    for t in (2, 3):
        part[t, here] = res[:, D * (3 - t):D * (4 - t)].reshape(2, RB, D)
        d2[t] = own_send(t)
    y_out[...] = (x[...].astype(F32) + mm(ot[...].reshape(D, N), wo[...], TN)).astype(BF16)

    outs = ((dwo_out, slice(0, D)), (dw_out, slice(2 * D, 3 * D)), (dw_out, slice(D, 2 * D)), (dw_out, slice(0, D)))
    for t in range(4):
        d2[t].wait_recv()
    for copy in ecopies:
        copy.wait()
    tot = (es[...] + er[0]) + (er[1] + er[2])
    dg_out[...] = tot[0:1]
    db_out[...] = tot[1:2]
    for t in range(4):
        link_copy(t).wait_recv()
        outs[t][0][:, outs[t][1]] = (part[t, sp] + rd2[t] + rl[t]).astype(BF16)
    for t in range(4):
        for copy in (d1[t], d2[t], link_copy(t)):
            copy.wait_send()

    @on_lead
    def _():
        for p in range(2):
            b[p].wait_send()
            c[p].wait_send()

    @on_second
    def _():
        for p in range(2):
            a[p].wait_send()


def write_out(y, dx, dw, dwo, dg, db, dt, y_o, dx_o, dw_o, dwo_o, dg_o, db_o, dt_o, sem):
    copies = [pltpu.make_async_copy(src, dst, sem.at[i]) for i, (src, dst) in enumerate(
        ((y, y_o), (dx, dx_o), (dw, dw_o), (dwo, dwo_o), (dg.at[0], dg_o), (db.at[0], db_o), (dt.at[0], dt_o)))]
    for copy in copies:
        copy.start()
    for copy in copies:
        copy.wait()


def local_step(x_rows, dy_rows, ln_gamma, ln_beta, w_qkv, w_out, temperature):
    hbm = pl.BlockSpec(memory_space=pltpu.HBM)
    vmem = pl.BlockSpec(memory_space=pltpu.VMEM)
    sds = jax.ShapeDtypeStruct
    outs = pl.pallas_call(
        kernel,
        out_shape=(sds((N, D), BF16), sds((N, D), BF16), sds((RB, 3 * D), BF16), sds((RB, D), BF16),
                   sds((1, D), F32), sds((1, D), F32), sds((1, 8), F32)),
        in_specs=[hbm] * 7,
        out_specs=(vmem,) * 7,
        scratch_shapes=[
            pltpu.VMEM((N, D), BF16),
            pltpu.VMEM((N, D), BF16),
            pltpu.VMEM((D, 3 * D), BF16),
            pltpu.VMEM((D, D), BF16),
            pltpu.VMEM((3 * D, D), BF16),
            pltpu.VMEM((N, D), BF16),
            pltpu.VMEM((2, GW, N), BF16),
            pltpu.VMEM((3, 2, GW, N), BF16),
            pltpu.VMEM((3, 2, GW, N), BF16),
            pltpu.VMEM((2, GW, N), BF16),
            pltpu.VMEM((2, GW, N), BF16),
            pltpu.VMEM((N, 1), F32),
            pltpu.VMEM((N, 1), F32),
            pltpu.VMEM((2 * D, 128), F32),
            pltpu.VMEM((2, 2, HD, PW), F32),
            pltpu.VMEM((2, 2, HD, PW), F32),
            pltpu.VMEM((2, 2, HD, PW), F32),
            pltpu.VMEM((2, 2, HD, PW), F32),
            pltpu.VMEM((2, 2, HD, PW), F32),
            pltpu.VMEM((2, 2, HD, PW), F32),
            pltpu.VMEM((2, GW, GW), BF16),
            pltpu.VMEM((2, GW, GW), BF16),
            pltpu.VMEM((5, 2, HD, PW), F32),
            pltpu.VMEM((4, 4, RB, D), F32),
            pltpu.VMEM((4, RB, D), F32),
            pltpu.VMEM((4, RB, D), F32),
            pltpu.VMEM((4, RB, D), F32),
            pltpu.VMEM((4, RB, D), F32),
            pltpu.VMEM((2, D), F32),
            pltpu.VMEM((3, 2, D), F32),
            pltpu.VMEM((1, D), F32),
            pltpu.VMEM((1, D), F32),
            pltpu.SMEM((8,), F32),
            pltpu.SemaphoreType.DMA((7,)),
            pltpu.SemaphoreType.DMA((NCH,)),
            pltpu.SemaphoreType.DMA((21,)),
            pltpu.SemaphoreType.DMA((21,)),
        ],
        compiler_params=pltpu.CompilerParams(collective_id=0, has_side_effects=True, vmem_limit_bytes=48 << 20),
        name="xca",
    )(*(pltpu.with_memory_space_constraint(a, pltpu.HBM)
        for a in (x_rows, dy_rows, ln_gamma, ln_beta, w_qkv, w_out, temperature)))
    return pl.pallas_call(
        write_out,
        out_shape=(sds((N, D), BF16), sds((N, D), BF16), sds((RB, 3 * D), BF16), sds((RB, D), BF16),
                   sds((D,), F32), sds((D,), F32), sds((8,), F32)),
        in_specs=[pl.BlockSpec(memory_space=pl.ANY)] * 7,
        out_specs=(hbm,) * 7,
        scratch_shapes=[pltpu.SemaphoreType.DMA((7,))],
        compiler_params=pltpu.CompilerParams(vmem_limit_bytes=1 << 20),
        name="write_out",
    )(*outs)


def solution(mesh):
    row_spec = P(('dp', 'sp'), None)
    full_mat = P(None, None)
    full_vec = P(None)
    part_vec = P('dp')
    return jax.shard_map(local_step, mesh=mesh,
                         in_specs=(row_spec, row_spec, full_vec, full_vec, full_mat, full_mat, full_vec),
                         out_specs=(row_spec, row_spec, row_spec, row_spec, part_vec, part_vec, part_vec),
                         check_vma=False)
```
